16 devices in a mesh: dp: 2 (over z), fo: 2 (over y), fi: 4 (over x, core).
Axes of the slice: x: 2, y: 2, z: 2, core: 2. Of those that a mesh axis runs over, the one named last changes fastest.
Arguments:
- X: bfloat16 [65536, 576], P(('dp', 'fo', 'fi'))
- dY: bfloat16 [65536, 576], P(('dp', 'fo', 'fi'))
- W1: bfloat16 [576, 1536], P(None, ('fo', 'fi'))
- W3: bfloat16 [576, 1536], P(None, ('fo', 'fi'))
- W2: bfloat16 [1536, 576], P(('fo', 'fi'))
- G: float32 [16, 3, 576, 1536], P(('dp', 'fo', 'fi'))
Outputs:
- output 1: bfloat16 [65536, 576], P(('dp', 'fo', 'fi'))
- output 2: float32 [3, 576, 1536], P(None, None, ('fo', 'fi'))
- output 3: float32 [16, 3, 576, 1536], P(('dp', 'fo', 'fi'))
All inputs are finite; a program needn't handle non-finite values.
Results may differ from the reference program's by a relative error of at most 0.0105754.
Values are sent between devices in bfloat16 or wider.
A program may use at most 1 GiB of HBM per device.

```python
import jax
import jax.numpy as jnp
from jax import lax

DEVS = 16
T = 4096
D = 576
FF = 1536


def setup_inputs(seed: int = 0) -> dict:
    key = jax.random.key(seed)
    k = jax.random.split(key, 6)
    n = DEVS * T
    x = jax.random.normal(k[0], (n, D), jnp.float32).astype(jnp.bfloat16)
    dy = jax.random.normal(k[1], (n, D), jnp.float32).astype(jnp.bfloat16)
    w1 = (jax.random.normal(k[2], (D, FF), jnp.float32) * D ** -0.5).astype(jnp.bfloat16)
    w3 = (jax.random.normal(k[3], (D, FF), jnp.float32) * D ** -0.5).astype(jnp.bfloat16)
    w2 = (jax.random.normal(k[4], (FF, D), jnp.float32) * FF ** -0.5).astype(jnp.bfloat16)
    g = jax.random.normal(k[5], (DEVS, 3, D, FF), jnp.float32)
    return {"X": x, "dY": dy, "W1": w1, "W3": w3, "W2": w2, "G": g}


def mlp_grads(x, dy, w1, w3, w2):
    a = jnp.dot(x, w1, preferred_element_type=jnp.float32)
    b = jnp.dot(x, w3, preferred_element_type=jnp.float32)
    s = jax.nn.sigmoid(a)
    sa = a * s
    h = (sa * b).astype(jnp.bfloat16)
    dh = jnp.dot(dy, w2.T, preferred_element_type=jnp.float32)
    da = (dh * b * (s * (1.0 + a * (1.0 - s)))).astype(jnp.bfloat16)
    db = (dh * sa).astype(jnp.bfloat16)
    dx = (jnp.dot(da, w1.T, preferred_element_type=jnp.float32)
          + jnp.dot(db, w3.T, preferred_element_type=jnp.float32)).astype(jnp.bfloat16)
    gw1 = jnp.dot(x.T, da, preferred_element_type=jnp.float32)
    gw3 = jnp.dot(x.T, db, preferred_element_type=jnp.float32)
    gw2 = jnp.dot(dy.T, h, preferred_element_type=jnp.float32)
    return dx, jnp.stack([gw1, gw3, gw2])


def reference(X, dY, W1, W3, W2, G):
    xs = X.reshape(DEVS, T, D)
    dys = dY.reshape(DEVS, T, D)
    dx, dwl = lax.map(lambda p: mlp_grads(p[0], p[1], W1, W3, W2), (xs, dys))
    dwn = jnp.sum(G.astype(jnp.bfloat16).astype(jnp.float32), axis=0)
    return dx.reshape(DEVS * T, D), dwn, dwl
```

```python
import jax
import jax.numpy as jnp
from jax import lax
from jax.experimental import pallas as pl
from jax.experimental.pallas import tpu as pltpu
from jax.sharding import PartitionSpec as P

bf16, f32 = jnp.bfloat16, jnp.float32
T, D, F = 4096, 576, 1536
FB, TB, RC = 384, 512, 16
NF, NT = F // FB, T // TB
NN = (((1,), (0,)), ((), ()))
NTD = (((1,), (1,)), ((), ()))
ANY = pl.BlockSpec(memory_space=pl.ANY)
VM = pl.BlockSpec(memory_space=pltpu.VMEM)


def dot(a, b):
    return lax.dot_general(a, b, NN, preferred_element_type=f32)


def kernel_a(x_hbm, dy_hbm, w_ref, wd_ref, dx_hbm, r_hbm,
             x, dy, acts, dd, hh, dxa, dxo, sx, sd, so, sdx):
    def xcp(t):
        return pltpu.make_async_copy(x_hbm.at[:, pl.ds(t * TB, TB)], x.at[t], sx.at[t])

    def dcp(t):
        return pltpu.make_async_copy(dy_hbm.at[:, pl.ds(t * TB, TB)], dy.at[t], sd.at[t])

    for t in range(NT):
        xcp(t).start()
        dcp(t).start()
    dd[1] = jnp.zeros(dd.shape[1:], bf16)

    def outcp(s, p):
        ts = pl.ds(pl.multiple_of(s % NT * TB, TB), TB)
        fs = pl.ds(pl.multiple_of(s // NT * FB, FB), FB)
        return [pltpu.make_async_copy(dd.at[p, pl.ds(0, FB)], r_hbm.at[0, fs, ts], so.at[p, 0]),
                pltpu.make_async_copy(dd.at[p, pl.ds(FB, FB)], r_hbm.at[1, fs, ts], so.at[p, 1]),
                pltpu.make_async_copy(hh.at[p], r_hbm.at[2, fs, ts], so.at[p, 2])]

    def fwd(f, t, p):
        fs = pl.ds(pl.multiple_of(f * FB, FB), FB)
        acts[p, 0] = dot(w_ref[0, fs, :], x[t])
        acts[p, 1] = dot(w_ref[1, fs, :], x[t])
        acts[p, 2] = dot(w_ref[2, fs, :], dy[t])

    def ew(p):
        for r in range(0, FB, RC):
            a, b, dh = (acts[p, k, r:r + RC, :] for k in range(3))
            s = 0.5 * jnp.tanh(0.5 * a) + 0.5
            sa = a * s
            hh[p, r:r + RC, :] = (sa * b).astype(bf16)
            dd[p, r:r + RC, :] = (dh * b * (s * (1.0 + a * (1.0 - s)))).astype(bf16)
            dd[p, FB + r:FB + r + RC, :] = (dh * sa).astype(bf16)

    def dxp(s, p):
        f, t = s // NT, s % NT
        dxa[t] = jnp.where(f == 0, 0.0, dxa[t]) + dot(wd_ref[f], dd[p])

    def body(i, c):
        s0 = 2 * i
        f, t0 = s0 // NT, s0 % NT
        s1, t1 = s0 + 1, t0 + 1

        @pl.when(f == 0)
        def _():
            for t in (t0, t1):
                xcp(t).wait()
                dcp(t).wait()

        @pl.when(i > 0)
        def _():
            for cp in outcp(s0 - 2, 0):
                cp.wait()

        fwd(f, t0, 0)
        ew(0)
        dxp(jnp.maximum(s0 - 1, 0), 1)

        @pl.when(i > 0)
        def _():
            for cp in outcp(s0 - 1, 1):
                cp.wait()

        for cp in outcp(s0, 0):
            cp.start()
        fwd(f, t1, 1)
        ew(1)
        dxp(s0, 0)
        for cp in outcp(s1, 1):
            cp.start()
        return c

    n = NF * NT
    lax.fori_loop(0, n // 2, body, 0)
    dxp(n - 1, 1)
    for p in (0, 1):
        for cp in outcp(n - 2 + p, p):
            cp.wait()

    def ocp(t, p):
        return pltpu.make_async_copy(dxo.at[p], dx_hbm.at[:, pl.ds(t * TB, TB)], sdx.at[p])

    for t in range(NT):
        p = t % 2
        if t >= 2:
            ocp(t - 2, p).wait()
        dxo[p] = dxa[t].astype(bf16)
        ocp(t, p).start()
    ocp(NT - 2, 0).wait()
    ocp(NT - 1, 1).wait()


def call_a(x, dy, w, wd):
    return pl.pallas_call(
        kernel_a,
        out_shape=(jax.ShapeDtypeStruct((D, T), bf16), jax.ShapeDtypeStruct((3, F, T), bf16)),
        in_specs=[ANY, ANY, VM, VM], out_specs=[ANY, ANY],
        scratch_shapes=[
            pltpu.VMEM((NT, D, TB), bf16), pltpu.VMEM((NT, D, TB), bf16),
            pltpu.VMEM((2, 3, FB, TB), f32), pltpu.VMEM((2, 2 * FB, TB), bf16),
            pltpu.VMEM((2, FB, TB), bf16), pltpu.VMEM((NT, D, TB), f32),
            pltpu.VMEM((2, D, TB), bf16),
            pltpu.SemaphoreType.DMA((NT,)), pltpu.SemaphoreType.DMA((NT,)),
            pltpu.SemaphoreType.DMA((2, 3)), pltpu.SemaphoreType.DMA((2,))],
        compiler_params=pltpu.CompilerParams(vmem_limit_bytes=63 << 20),
        cost_estimate=pl.CostEstimate(flops=70_000_000_000, bytes_accessed=60_000_000,
                                      transcendentals=0),
        name="fwd_dx")(x, dy, w, wd)


def kernel_b(x_ref, dy_ref, r_ref, o_ref):
    m = pl.program_id(0)

    @pl.when(m < 2)
    def _():
        o_ref[0] = lax.dot_general(x_ref[...], r_ref[0], NTD, preferred_element_type=f32)

    @pl.when(m == 2)
    def _():
        o_ref[0] = lax.dot_general(dy_ref[...], r_ref[0], NTD, preferred_element_type=f32)


def call_b(x, dy, r):
    bn = 512
    whole = pl.BlockSpec((D, T), lambda m, n: (0, 0), pipeline_mode=pl.Buffered(1))
    return pl.pallas_call(
        kernel_b,
        out_shape=jax.ShapeDtypeStruct((3, D, F), f32), grid=(3, F // bn),
        in_specs=[whole, whole, pl.BlockSpec((1, bn, T), lambda m, n: (m, n, 0))],
        out_specs=pl.BlockSpec((1, D, bn), lambda m, n: (m, 0, n)),
        compiler_params=pltpu.CompilerParams(vmem_limit_bytes=60 << 20),
        cost_estimate=pl.CostEstimate(flops=30_000_000_000, bytes_accessed=60_000_000,
                                      transcendentals=0),
        name="wgrad")(x, dy, r)


def solution(mesh):
    grp = ("fo", "fi")
    alla = ("dp", "fo", "fi")

    def local(x, dy, w1s, w3s, w2s, g):
        wt = jnp.stack([w1s.T, w3s.T, w2s])
        w = lax.all_gather(wt, grp, axis=1, tiled=True)
        w, g = lax.optimization_barrier((w, g))
        gs = lax.psum_scatter(g[0].astype(bf16), grp, scatter_dimension=2, tiled=True)
        wd = w[:2].reshape(2, NF, FB, D).transpose(1, 3, 0, 2).reshape(NF, D, 2 * FB)
        dx, r = call_a(x.T, dy.T, w, wd)
        gs, r = lax.optimization_barrier((gs, r))
        other = lax.ppermute(gs, "dp", [(0, 1), (1, 0)])
        dwl = call_b(x.T, dy.T, r)
        dwn = gs.astype(f32) + other.astype(f32)
        return dx.T, dwn, dwl[None]

    return jax.shard_map(
        local, mesh=mesh,
        in_specs=(P(alla, None), P(alla, None), P(None, grp), P(None, grp), P(grp, None),
                  P(alla, None, None, None)),
        out_specs=(P(alla, None), P(None, None, grp), P(alla, None, None, None)),
        check_vma=False)
```

```python
import jax
import jax.numpy as jnp
from jax import lax
from jax.experimental import pallas as pl
from jax.experimental.pallas import tpu as pltpu
from jax.sharding import PartitionSpec as P

bf16, f32 = jnp.bfloat16, jnp.float32
T, D, F = 4096, 576, 1536
FB, TB, RC = 384, 512, 16
NF, NT = F // FB, T // TB
NN = (((1,), (0,)), ((), ()))
NTD = (((1,), (1,)), ((), ()))
ANY = pl.BlockSpec(memory_space=pl.ANY)
VM = pl.BlockSpec(memory_space=pltpu.VMEM)


def dot(a, b):
    return lax.dot_general(a, b, NN, preferred_element_type=f32)


def kernel_a(x_hbm, dy_hbm, w1_hbm, w3_hbm, w2_hbm, g_hbm, dx_hbm, r_hbm, z_hbm,
             x, dy, acts, dd, hh, dxa, dxo, wg, wd, gst, sb, rb, r0, r1, r2, qb, fin, rz, zf, zr,
             sx, sd, so, sdx, sw, sg, ssem, rsem):
    zi, yi, fi = lax.axis_index("dp"), lax.axis_index("fo"), lax.axis_index("fi")
    xi, ci = fi // 2, fi % 2
    to_c = (zi, yi, xi * 2 + 1 - ci)
    to_x = (zi, yi, (1 - xi) * 2 + ci)
    to_y = (zi, 1 - yi, fi)
    to_z = (1 - zi, yi, fi)
    own = ci * 192
    half, other = own + zi * 96, own + (1 - zi) * 96

    def blk(yy, xx):
        return pl.ds(pl.multiple_of((yy * 2 + xx) * FB, FB), FB)

    def wrows(j, r, n):
        return wg.at[j, :, pl.ds(pl.multiple_of(r, 16), n), :]

    def piece(k, yy, xx):
        return rb.at[pl.ds(2 * k, 2), :, blk(yy, xx)]

    table = [
        (wrows(0, own, 192), wrows(0, own, 192), to_c),
        (wrows(0, own, 192), wrows(1, own, 192), to_x),
        (wrows(0, half, 96), wrows(2, half, 96), to_y),
        (wrows(1, own, 192), wrows(1, own, 192), to_c),
        (wrows(2, half, 96), wrows(2, half, 96), to_z),
        (wrows(2, half, 96), wrows(2, half, 96), to_c),
        (wrows(2, other, 96), wrows(2, other, 96), to_c),
        (wrows(1, half, 48), wrows(3, half, 48), to_y),
        (wrows(2, half + 48, 48), wrows(3, half + 48, 48), to_x),
        (wrows(3, half, 96), wrows(3, half, 96), to_z),
        (wrows(3, half, 96), wrows(3, half, 96), to_c),
        (wrows(3, other, 96), wrows(3, other, 96), to_c),
        (sb.at[pl.ds(0, 3)], rb.at[pl.ds(0, 3)], to_c),
        (sb.at[pl.ds(3, 3)], rb.at[pl.ds(3, 3)], to_c),
        (piece(0, 1 - yi, 1 - xi), r0.at[0], to_y),
        (piece(1, 1 - yi, 1 - xi), r0.at[1], to_y),
        (piece(2, 1 - yi, 1 - xi), r0.at[2], to_x),
        (piece(0, 1 - yi, xi), r1.at[0], to_y),
        (piece(1, 1 - yi, xi), r1.at[1], to_y),
        (piece(2, yi, 1 - xi), r1.at[2], to_x),
        (qb.at[0], r2.at[0], to_x),
        (qb.at[1], r2.at[1], to_x),
        (qb.at[2], r2.at[2], to_y),
        (fin.at[0], rz.at[0], to_z),
        (fin.at[1], rz.at[1], to_z),
        (fin.at[2], rz.at[2], to_z),
        (zf.at[pl.ds(0, 4)], zr.at[pl.ds(0, 4)], to_c),
        (zf.at[pl.ds(4, 2)], zr.at[pl.ds(4, 2)], to_c),
    ]

    def rc(k):
        src, dst, dev = table[k]
        return pltpu.make_async_remote_copy(src, dst, ssem.at[k], rsem.at[k], device_id=dev,
                                            device_id_type=pl.DeviceIdType.MESH)

    def start(*ks):
        for k in ks:
            rc(k).start()

    def arrived(*ks):
        for k in ks:
            rc(k).wait_recv()

    def xcp(t):
        return pltpu.make_async_copy(x_hbm.at[:, pl.ds(t * TB, TB)], x.at[t], sx.at[t])

    def dcp(t):
        return pltpu.make_async_copy(dy_hbm.at[:, pl.ds(t * TB, TB)], dy.at[t], sd.at[t])

    def gcp(i, side):
        return pltpu.make_async_copy(g_hbm.at[pl.ds(side * 6 + i * 3, 3)], gst.at[i], sg.at[i])

    wcps = [pltpu.make_async_copy(h, wg.at[0, m, pl.ds(pl.multiple_of(own, 192), 192), :], sw.at[m])
            for m, h in enumerate((w1_hbm, w3_hbm, w2_hbm))]
    for cp in wcps:
        cp.start()
    bar = pltpu.get_barrier_semaphore()
    for dev in (to_c, to_x, to_y, to_z):
        pl.semaphore_signal(bar, inc=1, device_id=dev, device_id_type=pl.DeviceIdType.MESH)
    xcp(0).start()
    dcp(0).start()
    xcp(1).start()
    dcp(1).start()
    for i in (0, 1):
        gcp(i, 1 - ci).start()
    for t in range(2, NT):
        xcp(t).start()
        dcp(t).start()
    dd[1] = jnp.zeros(dd.shape[1:], bf16)
    for cp in wcps:
        cp.wait()
    pl.semaphore_wait(bar, 4)
    start(0, 1, 2)

    def flip(j):
        for m in (0, 1):
            wd[j, :, m * FB:(m + 1) * FB] = wg[j, m].T

    def outcp(s, p):
        j = s // NT
        yj = yi + (j // 2) * (1 - 2 * yi)
        xj = xi + (j % 2) * (1 - 2 * xi)
        ts = pl.ds(pl.multiple_of(s % NT * TB, TB), TB)
        fs = pl.ds(pl.multiple_of((yj * 2 + xj) * FB, FB), FB)
        return [pltpu.make_async_copy(dd.at[p, pl.ds(0, FB)], r_hbm.at[0, fs, ts], so.at[p, 0]),
                pltpu.make_async_copy(dd.at[p, pl.ds(FB, FB)], r_hbm.at[1, fs, ts], so.at[p, 1]),
                pltpu.make_async_copy(hh.at[p], r_hbm.at[2, fs, ts], so.at[p, 2])]

    def fwd(f, t, p):
        acts[p, 0] = dot(wg[f, 0], x[t])
        acts[p, 1] = dot(wg[f, 1], x[t])
        acts[p, 2] = dot(wg[f, 2], dy[t])

    def ew(p):
        for r in range(0, FB, RC):
            a, b, dh = (acts[p, k, r:r + RC, :] for k in range(3))
            s = 0.5 * jnp.tanh(0.5 * a) + 0.5
            sa = a * s
            hh[p, r:r + RC, :] = (sa * b).astype(bf16)
            dd[p, r:r + RC, :] = (dh * b * (s * (1.0 + a * (1.0 - s)))).astype(bf16)
            dd[p, FB + r:FB + r + RC, :] = (dh * sa).astype(bf16)

    def dxp(s, p, first):
        t = s % NT
        if first:
            dxa[t] = dot(wd[0], dd[p])
        else:
            dxa[t] += dot(wd[s // NT], dd[p])

    def tiles(i, first, extra=None):
        s0 = 2 * i
        f, t0 = s0 // NT, s0 % NT

        def drain(p):
            for cp in outcp(s0 - 2 + p, p):
                cp.wait()

        if first:
            @pl.when(i > 0)
            def _():
                drain(0)
        else:
            drain(0)
        fwd(f, t0, 0)
        ew(0)
        if extra is not None:
            extra(0)
        dxp(s0 + NT - 1 if first else s0 - 1, 1, first)
        if first:
            @pl.when(i > 0)
            def _():
                drain(1)
        else:
            drain(1)
        for cp in outcp(s0, 0):
            cp.start()
        fwd(f, t0 + 1, 1)
        ew(1)
        if extra is not None:
            extra(1)
        dxp(s0, 0, first)
        for cp in outcp(s0 + 1, 1):
            cp.start()

    def need(i):
        for t in (2 * i, 2 * i + 1):
            xcp(t).wait()
            dcp(t).wait()

    def phase0a(i, c):
        need(i)
        gcp(i, 1 - ci).wait()

        def conv(h):
            for gr in range(3):
                for r in range(72 * h, 72 * h + 72, 24):
                    sb[i * 3 + gr, r:r + 24, :] = gst[i, gr, r:r + 24, :].astype(bf16)

        tiles(i, True, conv)

        @pl.when(i == 0)
        def _():
            start(12)

        @pl.when(i == 1)
        def _():
            start(13)

        gcp(i, ci).start()
        return c

    def phase0b(i, c):
        need(i + 2)
        gcp(i, ci).wait()

        @pl.when(i == 0)
        def _():
            arrived(12)

        @pl.when(i == 1)
        def _():
            arrived(13)
            start(14)
            arrived(2)
            start(4, 5, 8)

        def conv(h):
            for gr in range(3):
                for r in range(72 * h, 72 * h + 72, 24):
                    v = gst[i, gr, r:r + 24, :].astype(bf16).astype(f32)
                    v = v + rb[i * 3 + gr, r:r + 24, :].astype(f32)
                    rb[i * 3 + gr, r:r + 24, :] = v.astype(bf16)

        tiles(i + 2, True, conv)
        return c

    arrived(0)
    flip(0)
    lax.fori_loop(0, 2, phase0a, 0)
    lax.fori_loop(0, 2, phase0b, 0)
    start(15, 16)
    arrived(1)
    start(3, 7)
    arrived(3)
    flip(1)
    start(17, 18)

    def relay(k, yy, xx):
        qb[k] = (rb[2 * k:2 * k + 2, :, blk(yy, xx)].astype(f32) + r0[k].astype(f32)).astype(bf16)

    def group_sum(k):
        fin[k] = (rb[2 * k:2 * k + 2, :, blk(yi, xi)].astype(f32) + r1[k].astype(f32)
                  + r2[k].astype(f32)).astype(bf16)

    def total(k):
        zf[2 * k:2 * k + 2] = fin[k].astype(f32) + rz[k].astype(f32)

    def at5():
        arrived(14)
        relay(0, yi, 1 - xi)
        start(20)
        arrived(4)
        start(6)

    def at6():
        arrived(15)
        relay(1, yi, 1 - xi)
        start(21)

    def at7():
        arrived(7, 8)
        start(9, 10)
        arrived(16)
        relay(2, 1 - yi, xi)
        start(22, 19)

    def at8():
        arrived(5, 6)
        flip(2)

    def at10():
        arrived(17, 20)
        group_sum(0)
        start(23)

    def at11():
        arrived(18, 21)
        group_sum(1)
        start(24)
        arrived(9)
        start(11)

    def at12():
        arrived(10, 11)
        flip(3)
        arrived(19, 22)
        group_sum(2)
        start(25)

    def at15():
        arrived(23, 24)
        total(0)
        total(1)
        start(26)

    events = {5: at5, 6: at6, 7: at7, 8: at8, 10: at10, 11: at11, 12: at12, 15: at15}

    def phase1(i, c):
        for k, ev in events.items():
            pl.when(i == k)(ev)
        tiles(i, False)
        return c

    n = NF * NT
    lax.fori_loop(NT // 2, n // 2, phase1, 0)
    arrived(25)
    total(2)
    start(27)
    dxp(n - 1, 1, False)

    def ocp(t, p):
        return pltpu.make_async_copy(dxo.at[p], dx_hbm.at[:, pl.ds(t * TB, TB)], sdx.at[p])

    for t in range(NT):
        p = t % 2
        if t >= 2:
            ocp(t - 2, p).wait()
        dxo[p] = dxa[t].astype(bf16)
        ocp(t, p).start()
    zown = pltpu.make_async_copy(zf, z_hbm.at[pl.ds(ci * 6, 6)], sg.at[0])
    zoth = pltpu.make_async_copy(zr, z_hbm.at[pl.ds(6 - ci * 6, 6)], sg.at[1])
    zown.start()
    arrived(26, 27)
    zoth.start()
    for p in (0, 1):
        for cp in outcp(n - 2 + p, p):
            cp.wait()
    ocp(NT - 2, 0).wait()
    ocp(NT - 1, 1).wait()
    for k in range(len(table)):
        rc(k).wait_send()
    zown.wait()
    zoth.wait()


def call_a(x, dy, w1, w3, w2, g):
    part = (3, 2, 144, FB)
    return pl.pallas_call(
        kernel_a,
        out_shape=(jax.ShapeDtypeStruct((D, T), bf16), jax.ShapeDtypeStruct((3, F, T), bf16),
                   jax.ShapeDtypeStruct((12, 144, FB), f32)),
        in_specs=[ANY] * 6, out_specs=[ANY] * 3,
        scratch_shapes=[
            pltpu.VMEM((NT, D, TB), bf16), pltpu.VMEM((NT, D, TB), bf16),
            pltpu.VMEM((2, 3, FB, TB), f32), pltpu.VMEM((2, 2 * FB, TB), bf16),
            pltpu.VMEM((2, FB, TB), bf16), pltpu.VMEM((NT, D, TB), f32),
            pltpu.VMEM((2, D, TB), bf16),
            pltpu.VMEM((NF, 3, FB, D), bf16), pltpu.VMEM((NF, D, 2 * FB), bf16),
            pltpu.VMEM((2, 3, 144, F), f32), pltpu.VMEM((6, 144, F), bf16),
            pltpu.VMEM((6, 144, F), bf16),
            pltpu.VMEM(part, bf16), pltpu.VMEM(part, bf16), pltpu.VMEM(part, bf16),
            pltpu.VMEM(part, bf16), pltpu.VMEM(part, bf16), pltpu.VMEM(part, bf16),
            pltpu.VMEM((6, 144, FB), f32), pltpu.VMEM((6, 144, FB), f32),
            pltpu.SemaphoreType.DMA((NT,)), pltpu.SemaphoreType.DMA((NT,)),
            pltpu.SemaphoreType.DMA((2, 3)), pltpu.SemaphoreType.DMA((2,)),
            pltpu.SemaphoreType.DMA((3,)), pltpu.SemaphoreType.DMA((2,)),
            pltpu.SemaphoreType.DMA((28,)), pltpu.SemaphoreType.DMA((28,))],
        compiler_params=pltpu.CompilerParams(vmem_limit_bytes=67043328, collective_id=0,
                                             has_side_effects=True),
        cost_estimate=pl.CostEstimate(flops=40_000_000_000, bytes_accessed=60_000_000,
                                      transcendentals=0),
        name="fwd_dx")(x, dy, w1, w3, w2, g)


def kernel_b(x_ref, dy_ref, r_ref, o_ref):
    m = pl.program_id(0)

    @pl.when(m < 2)
    def _():
        o_ref[0] = lax.dot_general(x_ref[...], r_ref[0], NTD, preferred_element_type=f32)

    @pl.when(m == 2)
    def _():
        o_ref[0] = lax.dot_general(dy_ref[...], r_ref[0], NTD, preferred_element_type=f32)


def call_b(x, dy, r):
    bn = 512
    whole = pl.BlockSpec((D, T), lambda m, n: (0, 0), pipeline_mode=pl.Buffered(1))
    return pl.pallas_call(
        kernel_b,
        out_shape=jax.ShapeDtypeStruct((3, D, F), f32), grid=(3, F // bn),
        in_specs=[whole, whole, pl.BlockSpec((1, bn, T), lambda m, n: (m, n, 0))],
        out_specs=pl.BlockSpec((1, D, bn), lambda m, n: (m, 0, n)),
        compiler_params=pltpu.CompilerParams(vmem_limit_bytes=60 << 20),
        cost_estimate=pl.CostEstimate(flops=30_000_000_000, bytes_accessed=60_000_000,
                                      transcendentals=0),
        name="wgrad")(x, dy, r)


def solution(mesh):
    grp = ("fo", "fi")
    alla = ("dp", "fo", "fi")

    def local(x, dy, w1s, w3s, w2s, g):
        dx, r, z = call_a(x.T, dy.T, w1s.T, w3s.T, w2s, g.reshape(12, 144, F))
        dwl = call_b(x.T, dy.T, r)
        dwn = lax.dynamic_slice_in_dim(z.reshape(3, D, FB), lax.axis_index("fi") % 2 * 192, 192, 2)
        return dx.T, dwn, dwl[None]

    return jax.shard_map(
        local, mesh=mesh,
        in_specs=(P(alla, None), P(alla, None), P(None, grp), P(None, grp), P(grp, None),
                  P(alla, None, None, None)),
        out_specs=(P(alla, None), P(None, None, grp), P(alla, None, None, None)),
        check_vma=False)
```

```python
import jax
import jax.numpy as jnp
from jax import lax
from jax.experimental import pallas as pl
from jax.experimental.pallas import tpu as pltpu
from jax.sharding import PartitionSpec as P

bf16, f32 = jnp.bfloat16, jnp.float32
T, D, F = 4096, 576, 1536
FB, TB, RC = 384, 512, 16
NF, NT = F // FB, T // TB
NN = (((1,), (0,)), ((), ()))
NTD = (((1,), (1,)), ((), ()))
ANY = pl.BlockSpec(memory_space=pl.ANY)
VM = pl.BlockSpec(memory_space=pltpu.VMEM)


def dot(a, b):
    return lax.dot_general(a, b, NN, preferred_element_type=f32)


def kernel_a(x_hbm, dy_hbm, w1_hbm, w3_hbm, w2_hbm, g_hbm, dx_hbm, r_hbm, z_hbm,
             x, dy, acts, dda, ddb, hha, hhb, dxa, dxoa, dxob, wg, wd, gst, sb, rb, r0, r1, r2,
             qb, fin, rz, zf, zr,
             sx, sd, so, sdx, sw, sg, ssem, rsem):
    dd, hh, dxo = (dda, ddb), (hha, hhb), (dxoa, dxob)
    zi, yi, fi = lax.axis_index("dp"), lax.axis_index("fo"), lax.axis_index("fi")
    xi, ci = fi // 2, fi % 2
    to_c = (zi, yi, xi * 2 + 1 - ci)
    to_x = (zi, yi, (1 - xi) * 2 + ci)
    to_y = (zi, 1 - yi, fi)
    to_z = (1 - zi, yi, fi)
    own = ci * 192
    half, other = own + zi * 96, own + (1 - zi) * 96

    def blk(yy, xx):
        return pl.ds(pl.multiple_of((yy * 2 + xx) * FB, FB), FB)

    def wrows(j, r, n):
        return wg.at[j, :, pl.ds(pl.multiple_of(r, 16), n), :]

    def piece(k, yy, xx):
        return rb.at[pl.ds(2 * k, 2), :, blk(yy, xx)]

    table = [
        (wrows(0, own, 192), wrows(0, own, 192), to_c),
        (wrows(0, own, 192), wrows(1, own, 192), to_x),
        (wrows(0, half, 96), wrows(2, half, 96), to_y),
        (wrows(1, own, 192), wrows(1, own, 192), to_c),
        (wrows(2, half, 96), wrows(2, half, 96), to_z),
        (wrows(2, half, 96), wrows(2, half, 96), to_c),
        (wrows(2, other, 96), wrows(2, other, 96), to_c),
        (wrows(1, half, 48), wrows(3, half, 48), to_y),
        (wrows(2, half + 48, 48), wrows(3, half + 48, 48), to_x),
        (wrows(3, half, 96), wrows(3, half, 96), to_z),
        (wrows(3, half, 96), wrows(3, half, 96), to_c),
        (wrows(3, other, 96), wrows(3, other, 96), to_c),
        (sb.at[pl.ds(0, 3)], rb.at[pl.ds(0, 3)], to_c),
        (sb.at[pl.ds(3, 3)], rb.at[pl.ds(3, 3)], to_c),
        (piece(0, 1 - yi, 1 - xi), r0.at[0], to_y),
        (piece(1, 1 - yi, 1 - xi), r0.at[1], to_y),
        (piece(2, 1 - yi, 1 - xi), r0.at[2], to_x),
        (piece(0, 1 - yi, xi), r1.at[0], to_y),
        (piece(1, 1 - yi, xi), r1.at[1], to_y),
        (piece(2, yi, 1 - xi), r1.at[2], to_x),
        (qb.at[0], r2.at[0], to_x),
        (qb.at[1], r2.at[1], to_x),
        (qb.at[2], r2.at[2], to_y),
        (fin.at[0], rz.at[0], to_z),
        (fin.at[1], rz.at[1], to_z),
        (fin.at[2], rz.at[2], to_z),
        (zf.at[pl.ds(0, 4)], zr.at[pl.ds(0, 4)], to_c),
        (zf.at[pl.ds(4, 2)], zr.at[pl.ds(4, 2)], to_c),
    ]

    def rc(k):
        src, dst, dev = table[k]
        return pltpu.make_async_remote_copy(src, dst, ssem.at[k], rsem.at[k], device_id=dev,
                                            device_id_type=pl.DeviceIdType.MESH)

    def start(*ks):
        for k in ks:
            rc(k).start()

    def arrived(*ks):
        for k in ks:
            rc(k).wait_recv()

    def xcp(t):
        return pltpu.make_async_copy(x_hbm.at[:, pl.ds(t * TB, TB)], x.at[t], sx.at[t])

    def dcp(t):
        return pltpu.make_async_copy(dy_hbm.at[:, pl.ds(t * TB, TB)], dy.at[t], sd.at[t])

    def gcp(i, side):
        return pltpu.make_async_copy(g_hbm.at[pl.ds(side * 6 + i * 3, 3)], gst.at[i], sg.at[i])

    wcps = [pltpu.make_async_copy(h, wg.at[0, m, pl.ds(pl.multiple_of(own, 192), 192), :], sw.at[m])
            for m, h in enumerate((w1_hbm, w3_hbm, w2_hbm))]
    for cp in wcps:
        cp.start()
    bar = pltpu.get_barrier_semaphore()
    for dev in (to_c, to_x, to_y, to_z):
        pl.semaphore_signal(bar, inc=1, device_id=dev, device_id_type=pl.DeviceIdType.MESH)
    xcp(0).start()
    dcp(0).start()
    xcp(1).start()
    dcp(1).start()
    for i in (0, 1):
        gcp(i, 1 - ci).start()
    for t in range(2, NT):
        xcp(t).start()
        dcp(t).start()
    ddb[1] = jnp.zeros(ddb.shape[1:], bf16)
    for cp in wcps:
        cp.wait()
    pl.semaphore_wait(bar, 4)
    start(0, 1, 2)

    def flip(j):
        for m in (0, 1):
            wd[j, :, m * FB:(m + 1) * FB] = wg[j, m].T

    def outs(s0, q):
        j = s0 // NT
        yj = yi + (j // 2) * (1 - 2 * yi)
        xj = xi + (j % 2) * (1 - 2 * xi)
        fs = blk(yj, xj)
        res = []
        for p in (0, 1):
            ts = pl.ds(pl.multiple_of((s0 + p) % NT * TB, TB), TB)
            for m, src in enumerate((dd[p].at[q, pl.ds(0, FB)], dd[p].at[q, pl.ds(FB, FB)], hh[p].at[q])):
                res.append(pltpu.make_async_copy(src, r_hbm.at[m, fs, ts], so.at[q, p, m]))
        return res

    def fwd(f, t, p):
        acts[p, 0] = dot(wg[f, 0], x[t])
        acts[p, 1] = dot(wg[f, 1], x[t])
        acts[p, 2] = dot(wg[f, 2], dy[t])

    def ew(p, q):
        for r in range(0, FB, RC):
            a, b, dh = (acts[p, k, r:r + RC, :] for k in range(3))
            s = 0.5 * jnp.tanh(0.5 * a) + 0.5
            sa = a * s
            hh[p][q, r:r + RC, :] = (sa * b).astype(bf16)
            dd[p][q, r:r + RC, :] = (dh * b * (s * (1.0 + a * (1.0 - s)))).astype(bf16)
            dd[p][q, FB + r:FB + r + RC, :] = (dh * sa).astype(bf16)

    def ocp(s, q, p):
        ts = pl.ds(pl.multiple_of(s % NT * TB, TB), TB)
        return pltpu.make_async_copy(dxo[p].at[q], dx_hbm.at[:, ts], sdx.at[q, p])

    def dxp(s, q, p, first, o=None):
        t = s % NT
        if first:
            dxa[t] = dot(wd[0], dd[p][q])
            return
        v = dxa[t] + dot(wd[s // NT], dd[p][q])
        dxa[t] = v
        if o is not None:
            dxo[p][o] = v.astype(bf16)

    def tiles(i, first, extra=None, last=False):
        s0, q = 2 * i, i % 2
        f, t0 = s0 // NT, s0 % NT

        def drain():
            for cp in outs(s0 - 4, q):
                cp.wait()

        if first:
            pl.when(i > 1)(drain)
        else:
            drain()
        if last:
            @pl.when(i > 13)
            def _():
                ocp(s0 - 5, q, 1).wait()
                ocp(s0 - 4, q, 0).wait()

        o = q if last else None
        fwd(f, t0, 0)
        ew(0, q)
        if extra is not None:
            extra(0)
        dxp(s0 + NT - 1 if first else s0 - 1, 1 - q, 1, first, o)
        fwd(f, t0 + 1, 1)
        ew(1, q)
        if extra is not None:
            extra(1)
        dxp(s0, q, 0, first, o)
        for cp in outs(s0, q):
            cp.start()
        if last:
            ocp(s0 - 1, q, 1).start()
            ocp(s0, q, 0).start()

    def need(i):
        for t in (2 * i, 2 * i + 1):
            xcp(t).wait()
            dcp(t).wait()

    def phase0a(i, c):
        need(i)
        gcp(i, 1 - ci).wait()

        def conv(h):
            for gr in range(3):
                for r in range(72 * h, 72 * h + 72, 24):
                    sb[i * 3 + gr, r:r + 24, :] = gst[i, gr, r:r + 24, :].astype(bf16)

        tiles(i, True, conv)

        @pl.when(i == 0)
        def _():
            start(12)

        @pl.when(i == 1)
        def _():
            start(13)

        gcp(i, ci).start()
        return c

    def phase0b(i, c):
        need(i + 2)
        gcp(i, ci).wait()

        @pl.when(i == 0)
        def _():
            arrived(12)

        @pl.when(i == 1)
        def _():
            arrived(13)
            start(14)
            arrived(2)
            start(4, 5, 8)

        def conv(h):
            for gr in range(3):
                for r in range(72 * h, 72 * h + 72, 24):
                    v = gst[i, gr, r:r + 24, :].astype(bf16).astype(f32)
                    v = v + rb[i * 3 + gr, r:r + 24, :].astype(f32)
                    rb[i * 3 + gr, r:r + 24, :] = v.astype(bf16)

        tiles(i + 2, True, conv)
        return c

    arrived(0)
    flip(0)
    lax.fori_loop(0, 2, phase0a, 0)
    lax.fori_loop(0, 2, phase0b, 0)
    start(15, 16)
    arrived(1)
    start(3, 7)
    arrived(3)
    flip(1)
    start(17, 18)

    def relay(k, yy, xx):
        qb[k] = (rb[2 * k:2 * k + 2, :, blk(yy, xx)].astype(f32) + r0[k].astype(f32)).astype(bf16)

    def group_sum(k):
        fin[k] = (rb[2 * k:2 * k + 2, :, blk(yi, xi)].astype(f32) + r1[k].astype(f32)
                  + r2[k].astype(f32)).astype(bf16)

    def total(k):
        zf[2 * k:2 * k + 2] = fin[k].astype(f32) + rz[k].astype(f32)

    def at5():
        arrived(14)
        relay(0, yi, 1 - xi)
        start(20)
        arrived(4)
        start(6)

    def at6():
        arrived(15)
        relay(1, yi, 1 - xi)
        start(21)

    def at7():
        arrived(7, 8)
        start(9, 10)
        arrived(16)
        relay(2, 1 - yi, xi)
        start(22, 19)

    def at8():
        arrived(5, 6)
        flip(2)

    def at10():
        arrived(17, 20)
        group_sum(0)
        start(23)

    def at11():
        arrived(18, 21)
        group_sum(1)
        start(24)
        arrived(9)
        start(11)

    def at12():
        arrived(10, 11)
        flip(3)
        arrived(19, 22)
        group_sum(2)
        start(25)

    def at15():
        arrived(23, 24)
        total(0)
        total(1)
        start(26)

    events = {5: at5, 6: at6, 7: at7, 8: at8, 10: at10, 11: at11}

    def phase1(i, c):
        for k, ev in events.items():
            pl.when(i == k)(ev)
        tiles(i, False)
        return c

    def phase2(i, c):
        pl.when(i == 15)(at15)
        tiles(i, False, last=True)
        return c

    n = NF * NT
    lax.fori_loop(NT // 2, 12, phase1, 0)
    at12()
    lax.fori_loop(12, n // 2, phase2, 0)
    ocp(n - 5, 0, 1).wait()
    dxp(n - 1, 1, 1, False, 0)
    ocp(n - 1, 0, 1).start()
    zown = [pltpu.make_async_copy(zf.at[pl.ds(a, k)], z_hbm.at[pl.ds(ci * 6 + a, k)], sg.at[q])
            for q, (a, k) in enumerate(((0, 4), (4, 2)))]
    zoth = [pltpu.make_async_copy(zr.at[pl.ds(a, k)], z_hbm.at[pl.ds(6 - ci * 6 + a, k)], sw.at[q])
            for q, (a, k) in enumerate(((0, 4), (4, 2)))]
    zown[0].start()
    arrived(25)
    total(2)
    start(27)
    zown[1].start()
    arrived(26)
    zoth[0].start()
    for q in (0, 1):
        for cp in outs(n - 4 + 2 * q, q):
            cp.wait()
        ocp(n - 4 + 2 * q, q, 0).wait()
    ocp(n - 3, 1, 1).wait()
    for k in range(len(table)):
        rc(k).wait_send()
    arrived(27)
    zoth[1].start()
    ocp(n - 1, 0, 1).wait()
    for cp in zown + zoth:
        cp.wait()


def call_a(x, dy, w1, w3, w2, g):
    part = (3, 2, 144, FB)
    dma = pltpu.SemaphoreType.DMA
    return pl.pallas_call(
        kernel_a,
        out_shape=(jax.ShapeDtypeStruct((D, T), bf16), jax.ShapeDtypeStruct((3, F, T), bf16),
                   jax.ShapeDtypeStruct((12, 144, FB), f32)),
        in_specs=[ANY] * 6, out_specs=[ANY] * 3,
        scratch_shapes=[
            pltpu.VMEM((NT, D, TB), bf16), pltpu.VMEM((NT, D, TB), bf16),
            pltpu.VMEM((2, 3, FB, TB), f32), *[pltpu.VMEM((2, 2 * FB, TB), bf16)] * 2,
            *[pltpu.VMEM((2, FB, TB), bf16)] * 2, pltpu.VMEM((NT, D, TB), f32),
            *[pltpu.VMEM((2, D, TB), bf16)] * 2,
            pltpu.VMEM((NF, 3, FB, D), bf16), pltpu.VMEM((NF, D, 2 * FB), bf16),
            pltpu.VMEM((2, 3, 144, F), f32), *[pltpu.VMEM((6, 144, F), bf16)] * 2,
            *[pltpu.VMEM(part, bf16)] * 6, *[pltpu.VMEM((6, 144, FB), f32)] * 2,
            dma((NT,)), dma((NT,)), dma((2, 2, 3)), dma((2, 2)), dma((3,)), dma((2,)),
            dma((28,)), dma((28,))],
        compiler_params=pltpu.CompilerParams(vmem_limit_bytes=67043328, collective_id=0,
                                             has_side_effects=True),
        cost_estimate=pl.CostEstimate(flops=40_000_000_000, bytes_accessed=60_000_000,
                                      transcendentals=0),
        name="fwd_dx")(x, dy, w1, w3, w2, g)


def kernel_b(x_hbm, dy_hbm, r_hbm, dxi_hbm, z_hbm, o_hbm, dx_hbm, n_hbm,
             xy, r, o, dxb, zb, zt, sxk, srk, sdy, sr, so, sdx, sz, sn):
    ci = lax.axis_index("fi") % 2
    KC = T // 4

    def xk(k):
        return pltpu.make_async_copy(x_hbm.at[:, pl.ds(k * KC, KC)], xy.at[0, :, pl.ds(k * KC, KC)],
                                     sxk.at[k])

    def rk(k):
        return pltpu.make_async_copy(r_hbm.at[0, pl.ds(0, BN), pl.ds(k * KC, KC)],
                                     r.at[0, :, pl.ds(k * KC, KC)], srk.at[k])

    def rcp(m, n):
        return pltpu.make_async_copy(r_hbm.at[m, pl.ds(n * BN, BN), :], r.at[n], sr.at[n])

    def ocp(m, n):
        return pltpu.make_async_copy(o.at[n], o_hbm.at[m, :, pl.ds(n * BN, BN)], so.at[n])

    def ncp(m):
        return pltpu.make_async_copy(zt.at[m, pl.ds(pl.multiple_of(ci * 192, 192), 192), :],
                                     n_hbm.at[m], sn.at[m])

    dyc = pltpu.make_async_copy(dy_hbm, xy.at[1], sdy)
    dxin = pltpu.make_async_copy(dxi_hbm, dxb, sdx.at[0])
    dxout = pltpu.make_async_copy(dxb, dx_hbm, sdx.at[1])

    def zcp(m):
        return pltpu.make_async_copy(z_hbm.at[m], zb.at[m], sz.at[m])

    for k in range(4):
        xk(k).start()
        rk(k).start()
    rcp(0, 1).start()
    zcp(0).start()
    rcp(0, 2).start()
    for k in range(4):
        xk(k).wait()
        rk(k).wait()
        ks = slice(k * KC, (k + 1) * KC)
        v = lax.dot_general(xy[0, :, ks], r[0, :, ks], NTD, preferred_element_type=f32)
        o[0] = v if k == 0 else o[0] + v

    def ready(m, n):
        rcp(m, n).wait()

        @pl.when(m > 0)
        def _():
            ocp(m - 1, n).wait()

    def gw(m, n):
        o[n] = lax.dot_general(xy[m // 2], r[n], NTD, preferred_element_type=f32)

    def after(m, n):
        ocp(m, n).start()

        @pl.when(m < 2)
        def _():
            rcp(m + 1, n).start()

    def block(m, c):
        @pl.when(m == 2)
        def _():
            dyc.wait()
            dxin.wait()
            dxout.start()

        @pl.when(m > 0)
        def _():
            ready(m, 0)
            gw(m, 0)

        after(m, 0)
        ready(m, 1)
        zcp(m).wait()
        gw(m, 1)
        zt[m] = zb[m].T
        after(m, 1)
        ncp(m).start()

        @pl.when(m < 2)
        def _():
            zcp(m + 1).start()

        @pl.when(m == 0)
        def _():
            dyc.start()

        @pl.when(m == 1)
        def _():
            dxin.start()

        ready(m, 2)
        gw(m, 2)
        after(m, 2)
        return c

    lax.fori_loop(0, 3, block, 0)
    dxout.wait()
    for m in range(3):
        ncp(m).wait()
        ocp(2, m).wait()


BN = 512


def call_b(x, dy, r, dxi, z):
    dma = pltpu.SemaphoreType.DMA
    return pl.pallas_call(
        kernel_b,
        out_shape=(jax.ShapeDtypeStruct((3, D, F), f32), jax.ShapeDtypeStruct((D, T), bf16),
                   jax.ShapeDtypeStruct((3, 192, D), f32)),
        in_specs=[ANY] * 5, out_specs=[ANY] * 3,
        scratch_shapes=[
            pltpu.VMEM((2, D, T), bf16), pltpu.VMEM((3, BN, T), bf16), pltpu.VMEM((3, D, BN), f32),
            pltpu.VMEM((D, T), bf16), pltpu.VMEM((3, D, FB), f32), pltpu.VMEM((3, FB, D), f32),
            dma((4,)), dma((4,)), dma, dma((3,)), dma((3,)), dma((2,)), dma((3,)), dma((3,))],
        compiler_params=pltpu.CompilerParams(vmem_limit_bytes=60 << 20),
        cost_estimate=pl.CostEstimate(flops=30_000_000_000, bytes_accessed=60_000_000,
                                      transcendentals=0),
        name="wgrad")(x, dy, r, dxi, z)


def solution(mesh):
    grp = ("fo", "fi")
    alla = ("dp", "fo", "fi")

    def local(x, dy, w1s, w3s, w2s, g):
        dx, r, z = call_a(x.T, dy.T, w1s.T, w3s.T, w2s, g.reshape(12, 144, F))
        dwl, dx, dwn = call_b(x.T, dy.T, r, dx, z.reshape(3, D, FB))
        return dx.T, dwn.transpose(0, 2, 1), dwl[None]

    return jax.shard_map(
        local, mesh=mesh,
        in_specs=(P(alla, None), P(alla, None), P(None, grp), P(None, grp), P(grp, None),
                  P(alla, None, None, None)),
        out_specs=(P(alla, None), P(None, None, grp), P(alla, None, None, None)),
        check_vma=False)
```

```python
import jax
import jax.numpy as jnp
from jax import lax
from jax.experimental import pallas as pl
from jax.experimental.pallas import tpu as pltpu
from jax.sharding import PartitionSpec as P

bf16, f32 = jnp.bfloat16, jnp.float32
T, D, F = 4096, 576, 1536
FB, TB, RC = 384, 512, 16
NF, NT = F // FB, T // TB
NN = (((1,), (0,)), ((), ()))
NTD = (((1,), (1,)), ((), ()))
ANY = pl.BlockSpec(memory_space=pl.ANY)
VM = pl.BlockSpec(memory_space=pltpu.VMEM)


def dot(a, b):
    return lax.dot_general(a, b, NN, preferred_element_type=f32)


def kernel_a(x_hbm, dy_hbm, w1_hbm, w3_hbm, w2_hbm, g_hbm, dx_hbm, r_hbm, z_hbm, og_hbm,
             x, dy, acts, dda, ddb, dxa, dxoa, dxob, wg, wd, gst, sb, rb, r0, r1, r2,
             qb, fin, rz, zf, zr,
             sx, sd, so, sdx, sw, sg, ssem, rsem):
    dd, dxo = (dda, ddb), (dxoa, dxob)
    zi, yi, fi = lax.axis_index("dp"), lax.axis_index("fo"), lax.axis_index("fi")
    xi, ci = fi // 2, fi % 2
    to_c = (zi, yi, xi * 2 + 1 - ci)
    to_x = (zi, yi, (1 - xi) * 2 + ci)
    to_y = (zi, 1 - yi, fi)
    to_z = (1 - zi, yi, fi)
    own = ci * 192
    half, other = own + zi * 96, own + (1 - zi) * 96

    def blk(yy, xx):
        return pl.ds(pl.multiple_of((yy * 2 + xx) * FB, FB), FB)

    def wrows(j, r, n):
        return wg.at[j, :, pl.ds(pl.multiple_of(r, 16), n), :]

    def piece(k, yy, xx):
        return rb.at[pl.ds(2 * k, 2), :, blk(yy, xx)]

    table = [
        (wrows(0, own, 192), wrows(0, own, 192), to_c),
        (wrows(0, own, 192), wrows(1, own, 192), to_x),
        (wrows(0, half, 96), wrows(2, half, 96), to_y),
        (wrows(1, own, 192), wrows(1, own, 192), to_c),
        (wrows(2, half, 96), wrows(2, half, 96), to_z),
        (wrows(2, half, 96), wrows(2, half, 96), to_c),
        (wrows(2, other, 96), wrows(2, other, 96), to_c),
        (wrows(1, half, 48), wrows(3, half, 48), to_y),
        (wrows(2, half + 48, 48), wrows(3, half + 48, 48), to_x),
        (wrows(3, half, 96), wrows(3, half, 96), to_z),
        (wrows(3, half, 96), wrows(3, half, 96), to_c),
        (wrows(3, other, 96), wrows(3, other, 96), to_c),
    ]
    yo, xo = 1 - yi, 1 - xi
    fst, snd = (to_y, to_y, to_x), (to_x, to_x, to_y)
    far, near = ((yi, xo), (yi, xo), (yo, xi)), ((yo, xi), (yo, xi), (yi, xo))
    zp = (pl.ds(0, 4), pl.ds(4, 2))
    table += [(sb.at[pl.ds(k, 3)], rb.at[pl.ds(k, 3)], to_c) for k in (0, 3)]
    table += [(piece(k, yo, xo), r0.at[k], fst[k]) for k in range(3)]
    table += [(piece(k, *near[k]), r1.at[k], fst[k]) for k in range(3)]
    table += [(qb.at[k], r2.at[k], snd[k]) for k in range(3)]
    table += [(fin.at[k], rz.at[k], to_z) for k in range(3)]
    table += [(zf.at[sl], zr.at[sl], to_c) for sl in zp]

    def rc(k):
        src, dst, dev = table[k]
        return pltpu.make_async_remote_copy(src, dst, ssem.at[k], rsem.at[k], device_id=dev,
                                            device_id_type=pl.DeviceIdType.MESH)

    def start(*ks):
        for k in ks:
            rc(k).start()

    def arrived(*ks):
        for k in ks:
            rc(k).wait_recv()

    def xcp(t):
        return pltpu.make_async_copy(x_hbm.at[:, pl.ds(t * TB, TB)], x.at[t], sx.at[t])

    def dcp(t):
        return pltpu.make_async_copy(dy_hbm.at[:, pl.ds(t * TB, TB)], dy.at[t], sd.at[t])

    def gcp(i, side):
        return pltpu.make_async_copy(g_hbm.at[pl.ds(side * 6 + i * 3, 3)], gst.at[pl.ds(i * 3, 3)], sg.at[i])

    wcps = [pltpu.make_async_copy(h, wg.at[0, m, pl.ds(pl.multiple_of(own, 192), 192), :], sw.at[m])
            for m, h in enumerate((w1_hbm, w3_hbm, w2_hbm))]
    for cp in wcps:
        cp.start()
    bar = pltpu.get_barrier_semaphore()
    for dev in (to_c, to_x, to_y, to_z):
        pl.semaphore_signal(bar, inc=1, device_id=dev, device_id_type=pl.DeviceIdType.MESH)
    xcp(0).start()
    dcp(0).start()
    xcp(1).start()
    dcp(1).start()
    for i in (0, 1):
        gcp(i, 1 - ci).start()
    for t in range(2, NT):
        xcp(t).start()
        dcp(t).start()
    ddb[3] = jnp.zeros(ddb.shape[1:], bf16)
    for cp in wcps:
        cp.wait()
    pl.semaphore_wait(bar, 4)
    start(0, 1, 2)

    def flip(j):
        for m in (0, 1):
            wd[j, :, m * FB:(m + 1) * FB] = wg[j, m].T

    def outs(s0, q, first=False):
        j = s0 // NT
        yj = yi + (j // 2) * (1 - 2 * yi)
        xj = xi + (j % 2) * (1 - 2 * xi)
        fs = blk(yj, xj)
        w, m = (s0 // 2, 2) if first else (q, slice(None))
        return [pltpu.make_async_copy(
            dd[p].at[w, m], r_hbm.at[m, fs, pl.ds(pl.multiple_of((s0 + p) % NT * TB, TB), TB)],
            so.at[w, p]) for p in (0, 1)]

    def fwd(f, t, p):
        acts[p, 0] = dot(wg[f, 0], x[t])
        acts[p, 1] = dot(wg[f, 1], x[t])
        acts[p, 2] = dot(wg[f, 2], dy[t])

    def ew(p, w):
        for r in range(0, FB, RC):
            a, b, dh = (acts[p, k, r:r + RC, :] for k in range(3))
            s = 0.5 * jnp.tanh(0.5 * a) + 0.5
            sa = a * s
            dd[p][w, 2, r:r + RC, :] = (sa * b).astype(bf16)
            dd[p][w, 0, r:r + RC, :] = (dh * b * (s * (1.0 + a * (1.0 - s)))).astype(bf16)
            dd[p][w, 1, r:r + RC, :] = (dh * sa).astype(bf16)

    def ocp(s, q, p):
        ts = pl.ds(pl.multiple_of(s % NT * TB, TB), TB)
        return pltpu.make_async_copy(dxo[p].at[q], dx_hbm.at[:, ts], sdx.at[q, p])

    def dab(p, w):
        return dd[p][w, :2].reshape(2 * FB, TB)

    def dxp(s, q, p, first, o=None):
        t = s % NT
        if first:
            dxa[t] = dot(wd[0], dab(p, q))
            return
        v = dxa[t] + dot(wd[s // NT], dab(p, q))
        dxa[t] = v
        if o is not None:
            dxo[p][o] = v.astype(bf16)

    def tiles(i, first, extra=None, last=False):
        s0, q = 2 * i, i % 2
        w = i if first else q
        prev = (i + 3) % 4 if first else 1 - q if last else 1 - q + 2 * ((11 - i) // 7)
        f, t0 = s0 // NT, s0 % NT

        if not first:
            @pl.when(i > 5)
            def _():
                for cp in outs(s0 - 4, q):
                    cp.wait()

        if last:
            @pl.when(i > 13)
            def _():
                ocp(s0 - 5, q, 1).wait()
                ocp(s0 - 4, q, 0).wait()

        o = q if last else None
        fwd(f, t0, 0)
        ew(0, w)
        if extra is not None:
            extra(0)
        dxp(s0 + NT - 1 if first else s0 - 1, prev, 1, first, o)
        fwd(f, t0 + 1, 1)
        ew(1, w)
        if extra is not None:
            extra(1)
        dxp(s0, w, 0, first, o)
        for cp in outs(s0, q, first):
            cp.start()
        if last:
            ocp(s0 - 1, q, 1).start()
            ocp(s0, q, 0).start()

    def need(i):
        for t in (2 * i, 2 * i + 1):
            xcp(t).wait()
            dcp(t).wait()

    def phase0a(i, c):
        need(i)
        gcp(i, 1 - ci).wait()

        def conv(h):
            for gr in range(3):
                for r in range(72 * h, 72 * h + 72, 24):
                    sb[i * 3 + gr, r:r + 24, :] = gst[i * 3 + gr, r:r + 24, :].astype(bf16)

        tiles(i, True, conv)

        @pl.when(i == 0)
        def _():
            start(12)

        @pl.when(i == 1)
        def _():
            start(13)

        gcp(i, ci).start()
        return c

    def phase0b(i, c):
        need(i + 2)
        gcp(i, ci).wait()

        @pl.when(i == 0)
        def _():
            arrived(12)

        @pl.when(i == 1)
        def _():
            arrived(13)
            start(14)
            arrived(2)
            start(4, 5, 8)

        def conv(h):
            for gr in range(3):
                for r in range(72 * h, 72 * h + 72, 24):
                    v = gst[i * 3 + gr, r:r + 24, :].astype(bf16).astype(f32)
                    v = v + rb[i * 3 + gr, r:r + 24, :].astype(f32)
                    rb[i * 3 + gr, r:r + 24, :] = v.astype(bf16)

        tiles(i + 2, True, conv)
        return c

    arrived(0)
    flip(0)
    lax.fori_loop(0, 2, phase0a, 0)
    lax.fori_loop(0, 2, phase0b, 0)
    start(15, 16)
    def own_grads(ts):
        return sum(lax.dot_general(x[t], dab(t % 2, t // 2), NTD, preferred_element_type=f32)
                   for t in ts).reshape(4, 144, 2 * FB)

    og = gst.at[pl.ds(0, 4), :, pl.ds(0, 2 * FB)]
    og[...] = own_grads(range(4))
    arrived(1)
    start(3, 7)
    og[...] += own_grads(range(4, NT))
    ogc = pltpu.make_async_copy(og, og_hbm, sw.at[2])
    ogc.start()
    for i in range(NT // 2):
        for cp in outs(2 * i, 0, True):
            cp.wait()
    arrived(3)
    flip(1)
    start(17, 18)

    def relay(k):
        qb[k] = (rb[2 * k:2 * k + 2, :, blk(*far[k])].astype(f32) + r0[k].astype(f32)).astype(bf16)

    def group_sum(k):
        fin[k] = (rb[2 * k:2 * k + 2, :, blk(yi, xi)].astype(f32) + r1[k].astype(f32)
                  + r2[k].astype(f32)).astype(bf16)

    def total(k):
        zf[2 * k:2 * k + 2] = fin[k].astype(f32) + rz[k].astype(f32)

    def at5():
        arrived(14)
        relay(0)
        start(20)
        arrived(4)
        start(6)

    def at6():
        arrived(15)
        relay(1)
        start(21)

    def at7():
        arrived(7, 8)
        start(9, 10)
        arrived(16)
        relay(2)
        start(22, 19)

    def at8():
        arrived(5, 6)
        flip(2)

    def at10():
        arrived(17, 20)
        group_sum(0)
        start(23)

    def at11():
        arrived(18, 21)
        group_sum(1)
        start(24)
        arrived(9)
        start(11)

    def at12():
        arrived(10, 11)
        flip(3)
        arrived(19, 22)
        group_sum(2)
        start(25)

    def zown(q):
        sl = zp[q]
        return pltpu.make_async_copy(zf.at[sl], z_hbm.at[pl.ds(ci * 6 + sl.start, sl.size)], sg.at[q])

    def at15():
        arrived(23, 24)
        total(0)
        total(1)
        start(26)
        zown(0).start()

    events = {5: at5, 6: at6, 7: at7, 8: at8, 10: at10, 11: at11}

    def phase1(i, c):
        for k, ev in events.items():
            pl.when(i == k)(ev)
        tiles(i, False)
        return c

    def phase2(i, c):
        pl.when(i == 15)(at15)
        tiles(i, False, last=True)
        return c

    n = NF * NT
    lax.fori_loop(NT // 2, 12, phase1, 0)
    at12()
    lax.fori_loop(12, n // 2, phase2, 0)
    ocp(n - 5, 0, 1).wait()
    dxp(n - 1, 1, 1, False, 0)
    ocp(n - 1, 0, 1).start()
    zoth = [pltpu.make_async_copy(zr.at[sl], z_hbm.at[pl.ds(6 - ci * 6 + sl.start, sl.size)], sw.at[q])
            for q, sl in enumerate(zp)]
    arrived(25)
    total(2)
    start(27)
    zown(1).start()
    arrived(26)
    zoth[0].start()
    for q in (0, 1):
        for cp in outs(n - 4 + 2 * q, q):
            cp.wait()
        ocp(n - 4 + 2 * q, q, 0).wait()
    ocp(n - 3, 1, 1).wait()
    for k in range(len(table)):
        rc(k).wait_send()
    arrived(27)
    zoth[1].start()
    ocp(n - 1, 0, 1).wait()
    for cp in zoth + [zown(0), zown(1), ogc]:
        cp.wait()


def call_a(x, dy, w1, w3, w2, g):
    part = (3, 2, 144, FB)
    dma = pltpu.SemaphoreType.DMA
    return pl.pallas_call(
        kernel_a,
        out_shape=(jax.ShapeDtypeStruct((D, T), bf16), jax.ShapeDtypeStruct((3, F, T), bf16),
                   jax.ShapeDtypeStruct((12, 144, FB), f32),
                   jax.ShapeDtypeStruct((4, 144, 2 * FB), f32)),
        in_specs=[ANY] * 6, out_specs=[ANY] * 4,
        scratch_shapes=[
            pltpu.VMEM((NT, D, TB), bf16), pltpu.VMEM((NT, D, TB), bf16),
            pltpu.VMEM((2, 3, FB, TB), f32), *[pltpu.VMEM((4, 3, FB, TB), bf16)] * 2,
            pltpu.VMEM((NT, D, TB), f32),
            *[pltpu.VMEM((2, D, TB), bf16)] * 2,
            pltpu.VMEM((NF, 3, FB, D), bf16), pltpu.VMEM((NF, D, 2 * FB), bf16),
            pltpu.VMEM((6, 144, F), f32), *[pltpu.VMEM((6, 144, F), bf16)] * 2,
            *[pltpu.VMEM(part, bf16)] * 6, *[pltpu.VMEM((6, 144, FB), f32)] * 2,
            dma((NT,)), dma((NT,)), dma((4, 2)), dma((2, 2)), dma((3,)), dma((2,)),
            dma((28,)), dma((28,))],
        compiler_params=pltpu.CompilerParams(vmem_limit_bytes=67043328, collective_id=0,
                                             has_side_effects=True),
        name="fwd_dx")(x, dy, w1, w3, w2, g)


def kernel_b(x_hbm, dy_hbm, r_hbm, dxi_hbm, z_hbm, og_hbm, o_hbm, dx_hbm, n_hbm,
             xy, r0, r, o0, o, dxb, ogb, zb, zt, sx, s0, so0, sdy, sr, so, sdx, sog, sz, sn):
    yi, fi = lax.axis_index("fo"), lax.axis_index("fi")
    xi, ci = fi // 2, fi % 2

    def cols(b, n):
        return pl.ds(pl.multiple_of(b * n, n), n)

    def tri(src, dst, sem):
        return pltpu.make_async_copy(src, dst, sem)

    nb = cols(yi * 2 + 1 - xi, FB)
    mine = cols(yi * 2 + xi, FB)
    ks = [pl.ds(k * KC, KC) for k in range(T // KC)]
    first = [[tri(x_hbm.at[:, k], xy.at[0, :, k], sx.at[q])]
             + [tri(r_hbm.at[m, nb, k], r0.at[pl.ds(m * FB, FB), k], s0.at[m, q]) for m in (0, 1)]
             for q, k in enumerate(ks)]
    o0c = [tri(o0.at[:, pl.ds(m * FB, FB)], o_hbm.at[m, :, nb], so0.at[m]) for m in (0, 1)]
    dyc = tri(dy_hbm, xy.at[1], sdy)
    dxin, dxout = tri(dxi_hbm, dxb, sdx.at[0]), tri(dxb, dx_hbm, sdx.at[1])
    ogin = tri(og_hbm, ogb, sog.at[2])
    ogout = [tri(ogb.at[:, pl.ds(m * FB, FB)], o_hbm.at[m, :, mine], sog.at[m]) for m in (0, 1)]

    def place(s):
        return s - s // 3, cols((1 - s // 2) * (1 - yi) + s // 3, BN)

    def rcp(s):
        m, c = place(s)
        return tri(r_hbm.at[m, c, :], r.at[s % 2], sr.at[s % 2])

    def ocp(s):
        m, c = place(s)
        return tri(o.at[s % 2], o_hbm.at[m, :, c], so.at[s % 2])

    def zcp(m):
        return tri(z_hbm.at[m], zb.at[m], sz.at[m])

    def ncp(m):
        return tri(zt.at[m, cols(ci, FB // 2), :], n_hbm.at[m], sn.at[m])

    for cps in first:
        for cp in cps:
            cp.start()
    rcp(0).start()
    rcp(1).start()
    for m in range(3):
        zcp(m).start()
    dyc.start()
    zb[3] = jnp.zeros(zb.shape[1:], f32)
    for q, cps in enumerate(first):
        for cp in cps:
            cp.wait()
        v = lax.dot_general(xy[0, :, ks[q]], r0[:, ks[q]], NTD, preferred_element_type=f32)
        o0[...] = v if q == 0 else o0[...] + v
    for cp in o0c:
        cp.start()

    def step(s, c):
        pl.when(s == 2)(dyc.wait)

        @pl.when(s == 3)
        def _():
            dxin.wait()
            dxout.start()
            ogin.wait()
            for cp in ogout:
                cp.start()

        @pl.when(s > 0)
        def _():
            zcp(s - 1).wait()

        rcp(s).wait()
        pl.when(s > 1)(ocp(s - 2).wait)
        o[s % 2] = lax.dot_general(xy[s // 2], r[s % 2], NTD, preferred_element_type=f32)
        zt[(s + 3) % 4] = zb[(s + 3) % 4].T
        ocp(s).start()

        @pl.when(s > 0)
        def _():
            ncp(s - 1).start()

        @pl.when(s < 2)
        def _():
            rcp(s + 2).start()

        pl.when(s == 0)(dxin.start)
        pl.when(s == 1)(ogin.start)
        return c

    lax.fori_loop(0, 4, step, 0)
    for cp in o0c + ogout + [dxout, ocp(2), ocp(3)] + [ncp(m) for m in range(3)]:
        cp.wait()


BN, KC = 2 * FB, 1024


def call_b(x, dy, r, dxi, z, og):
    dma = pltpu.SemaphoreType.DMA
    return pl.pallas_call(
        kernel_b,
        out_shape=(jax.ShapeDtypeStruct((3, D, F), f32), jax.ShapeDtypeStruct((D, T), bf16),
                   jax.ShapeDtypeStruct((3, FB // 2, D), f32)),
        in_specs=[ANY] * 6, out_specs=[ANY] * 3,
        scratch_shapes=[
            pltpu.VMEM((2, D, T), bf16), pltpu.VMEM((BN, T), bf16), pltpu.VMEM((2, BN, T), bf16),
            pltpu.VMEM((D, BN), f32), pltpu.VMEM((2, D, BN), f32), pltpu.VMEM((D, T), bf16),
            pltpu.VMEM((D, BN), f32), pltpu.VMEM((4, D, FB), f32), pltpu.VMEM((4, FB, D), f32),
            dma((4,)), dma((2, 4)), dma((2,)), dma, dma((2,)), dma((2,)), dma((2,)), dma((3,)),
            dma((3,)), dma((3,))],
        compiler_params=pltpu.CompilerParams(vmem_limit_bytes=60 << 20),
        name="wgrad")(x, dy, r, dxi, z, og)


def solution(mesh):
    grp = ("fo", "fi")
    alla = ("dp", "fo", "fi")

    def local(x, dy, w1s, w3s, w2s, g):
        dx, r, z, og = call_a(x.T, dy.T, w1s.T, w3s.T, w2s, g.reshape(12, 144, F))
        dwl, dx, dwn = call_b(x.T, dy.T, r, dx, z.reshape(3, D, FB), og.reshape(D, BN))
        return dx.T, dwn.transpose(0, 2, 1), dwl[None]

    return jax.shard_map(
        local, mesh=mesh,
        in_specs=(P(alla, None), P(alla, None), P(None, grp), P(None, grp), P(grp, None),
                  P(alla, None, None, None)),
        out_specs=(P(alla, None), P(None, None, grp), P(alla, None, None, None)),
        check_vma=False)
```

```python
import jax
import jax.numpy as jnp
from jax import lax
from jax.experimental import pallas as pl
from jax.experimental.pallas import tpu as pltpu
from jax.sharding import PartitionSpec as P

bf16, f32 = jnp.bfloat16, jnp.float32
T, D, F = 4096, 576, 1536
FB, TB, RC = 384, 512, 16
NF, NT = F // FB, T // TB
NN = (((1,), (0,)), ((), ()))
NTD = (((1,), (1,)), ((), ()))
ANY = pl.BlockSpec(memory_space=pl.ANY)
VM = pl.BlockSpec(memory_space=pltpu.VMEM)


def dot(a, b):
    return lax.dot_general(a, b, NN, preferred_element_type=f32)


def kernel_a(x_hbm, dy_hbm, w1_hbm, w3_hbm, w2_hbm, g_hbm, dx_hbm, r_hbm, z_hbm, og_hbm,
             x, dy, acts, dda, ddb, dxa, dxoa, dxob, wg, gst, sb, rb, r0, r1, r2,
             qb, fin, rz, zf, zr,
             sx, sd, so, sdx, sw, sg, ssem, rsem):
    dd, dxo = (dda, ddb), (dxoa, dxob)
    zi, yi, fi = lax.axis_index("dp"), lax.axis_index("fo"), lax.axis_index("fi")
    xi, ci = fi // 2, fi % 2
    to_c = (zi, yi, xi * 2 + 1 - ci)
    to_x = (zi, yi, (1 - xi) * 2 + ci)
    to_y = (zi, 1 - yi, fi)
    to_z = (1 - zi, yi, fi)
    own = ci * 192
    half, other = own + zi * 96, own + (1 - zi) * 96

    def blk(yy, xx):
        return pl.ds(pl.multiple_of((yy * 2 + xx) * FB, FB), FB)

    def wrows(j, r, n):
        return wg.at[j, :, pl.ds(pl.multiple_of(r, 16), n), :]

    def piece(k, yy, xx):
        return rb.at[pl.ds(2 * k, 2), :, blk(yy, xx)]

    table = [
        (wrows(0, own, 192), wrows(0, own, 192), to_c),
        (wrows(0, own, 192), wrows(1, own, 192), to_x),
        (wrows(0, half, 96), wrows(2, half, 96), to_y),
        (wrows(1, own, 192), wrows(1, own, 192), to_c),
        (wrows(2, half, 96), wrows(2, half, 96), to_z),
        (wrows(2, half, 96), wrows(2, half, 96), to_c),
        (wrows(2, other, 96), wrows(2, other, 96), to_c),
        (wrows(1, half, 48), wrows(3, half, 48), to_y),
        (wrows(2, half + 48, 48), wrows(3, half + 48, 48), to_x),
        (wrows(3, half, 96), wrows(3, half, 96), to_z),
        (wrows(3, half, 96), wrows(3, half, 96), to_c),
        (wrows(3, other, 96), wrows(3, other, 96), to_c),
    ]
    yo, xo = 1 - yi, 1 - xi
    fst, snd = (to_y, to_y, to_x), (to_x, to_x, to_y)
    far, near = ((yi, xo), (yi, xo), (yo, xi)), ((yo, xi), (yo, xi), (yi, xo))
    zp = (pl.ds(0, 4), pl.ds(4, 2))
    table += [(sb.at[pl.ds(k, 3)], rb.at[pl.ds(k, 3)], to_c) for k in (0, 3)]
    table += [(piece(k, yo, xo), r0.at[k], fst[k]) for k in range(3)]
    table += [(piece(k, *near[k]), r1.at[k], fst[k]) for k in range(3)]
    table += [(qb.at[k], r2.at[k], snd[k]) for k in range(3)]
    table += [(fin.at[k], rz.at[k], to_z) for k in range(3)]
    table += [(zf.at[sl], zr.at[sl], to_c) for sl in zp]

    def rc(k):
        src, dst, dev = table[k]
        return pltpu.make_async_remote_copy(src, dst, ssem.at[k], rsem.at[k], device_id=dev,
                                            device_id_type=pl.DeviceIdType.MESH)

    def start(*ks):
        for k in ks:
            rc(k).start()

    def arrived(*ks):
        for k in ks:
            rc(k).wait_recv()

    def xcp(t):
        return pltpu.make_async_copy(x_hbm.at[:, pl.ds(t * TB, TB)], x.at[t], sx.at[t])

    def dcp(t):
        return pltpu.make_async_copy(dy_hbm.at[:, pl.ds(t * TB, TB)], dy.at[t], sd.at[t])

    def gcp(i, side):
        return pltpu.make_async_copy(g_hbm.at[pl.ds(side * 6 + i * 3, 3)], gst.at[pl.ds(i * 3, 3)], sg.at[i])

    wcps = [pltpu.make_async_copy(h, wg.at[0, m, pl.ds(pl.multiple_of(own, 192), 192), :], sw.at[m])
            for m, h in enumerate((w1_hbm, w3_hbm, w2_hbm))]
    for cp in wcps:
        cp.start()
    bar = pltpu.get_barrier_semaphore()
    for dev in (to_c, to_x, to_y, to_z):
        pl.semaphore_signal(bar, inc=1, device_id=dev, device_id_type=pl.DeviceIdType.MESH)
    xcp(0).start()
    dcp(0).start()
    xcp(1).start()
    dcp(1).start()
    for i in (0, 1):
        gcp(i, 1 - ci).start()
    for t in range(2, NT):
        xcp(t).start()
        dcp(t).start()
    ddb[3] = jnp.zeros(ddb.shape[1:], bf16)
    for cp in wcps:
        cp.wait()
    pl.semaphore_wait(bar, 4)
    start(0, 1, 2)

    def outs(s0, q, first=False):
        j = s0 // NT
        yj = yi + (j // 2) * (1 - 2 * yi)
        xj = xi + (j % 2) * (1 - 2 * xi)
        fs = blk(yj, xj)
        w, m = (s0 // 2, 2) if first else (q, slice(None))
        return [pltpu.make_async_copy(
            dd[p].at[w, m], r_hbm.at[m, fs, pl.ds(pl.multiple_of((s0 + p) % NT * TB, TB), TB)],
            so.at[w, p]) for p in (0, 1)]

    def fwd(f, t, p):
        acts[p, 0] = dot(wg[f, 0], x[t])
        acts[p, 1] = dot(wg[f, 1], x[t])
        acts[p, 2] = dot(wg[f, 2], dy[t])

    def ew(p, w):
        for r in range(0, FB, RC):
            a, b, dh = (acts[p, k, r:r + RC, :] for k in range(3))
            s = 0.5 * jnp.tanh(0.5 * a) + 0.5
            sa = a * s
            dd[p][w, 2, r:r + RC, :] = (sa * b).astype(bf16)
            dd[p][w, 0, r:r + RC, :] = (dh * b * (s * (1.0 + a * (1.0 - s)))).astype(bf16)
            dd[p][w, 1, r:r + RC, :] = (dh * sa).astype(bf16)

    def ocp(s, q, p):
        ts = pl.ds(pl.multiple_of(s % NT * TB, TB), TB)
        return pltpu.make_async_copy(dxo[p].at[q], dx_hbm.at[:, ts], sdx.at[q, p])

    def tdot(j, b):
        return lax.dot_general(wg[j, :2].reshape(2 * FB, D), b, (((0,), (0,)), ((), ())),
                               preferred_element_type=f32)

    def dab(p, w):
        return dd[p][w, :2].reshape(2 * FB, TB)

    def dxp(s, q, p, first, o=None):
        t = s % NT
        if first:
            dxa[t] = tdot(0, dab(p, q))
            return
        v = dxa[t] + tdot(s // NT, dab(p, q))
        dxa[t] = v
        if o is not None:
            dxo[p][o] = v.astype(bf16)

    def tiles(i, first, extra=None, last=False):
        s0, q = 2 * i, i % 2
        w = i if first else q
        prev = (i + 3) % 4 if first else 1 - q if last else 1 - q + 2 * ((11 - i) // 7)
        f, t0 = s0 // NT, s0 % NT

        if not first:
            @pl.when(i > 5)
            def _():
                for cp in outs(s0 - 4, q):
                    cp.wait()

        if last:
            @pl.when(i > 13)
            def _():
                ocp(s0 - 5, q, 1).wait()
                ocp(s0 - 4, q, 0).wait()

        o = q if last else None
        fwd(f, t0, 0)
        ew(0, w)
        if extra is not None:
            extra(0)
        dxp(s0 + NT - 1 if first else s0 - 1, prev, 1, first, o)
        fwd(f, t0 + 1, 1)
        ew(1, w)
        if extra is not None:
            extra(1)
        dxp(s0, w, 0, first, o)
        for cp in outs(s0, q, first):
            cp.start()
        if last:
            ocp(s0 - 1, q, 1).start()
            ocp(s0, q, 0).start()

    def need(i):
        for t in (2 * i, 2 * i + 1):
            xcp(t).wait()
            dcp(t).wait()

    def phase0a(i, c):
        need(i)
        gcp(i, 1 - ci).wait()

        def conv(h):
            for gr in range(3):
                for r in range(72 * h, 72 * h + 72, 24):
                    sb[i * 3 + gr, r:r + 24, :] = gst[i * 3 + gr, r:r + 24, :].astype(bf16)

        tiles(i, True, conv)

        @pl.when(i == 0)
        def _():
            start(12)

        @pl.when(i == 1)
        def _():
            start(13)

        gcp(i, ci).start()
        return c

    def phase0b(i, c):
        need(i + 2)
        gcp(i, ci).wait()

        @pl.when(i == 0)
        def _():
            arrived(12)

        @pl.when(i == 1)
        def _():
            arrived(13)
            start(14)
            arrived(2)
            start(4, 5, 8)

        def conv(h):
            for gr in range(3):
                for r in range(72 * h, 72 * h + 72, 24):
                    v = gst[i * 3 + gr, r:r + 24, :].astype(bf16).astype(f32)
                    v = v + rb[i * 3 + gr, r:r + 24, :].astype(f32)
                    rb[i * 3 + gr, r:r + 24, :] = v.astype(bf16)

        tiles(i + 2, True, conv)
        return c

    arrived(0)
    lax.fori_loop(0, 2, phase0a, 0)
    lax.fori_loop(0, 2, phase0b, 0)
    start(15, 16)
    def own_grads(ts):
        return sum(lax.dot_general(x[t], dab(t % 2, t // 2), NTD, preferred_element_type=f32)
                   for t in ts).reshape(4, 144, 2 * FB)

    og = gst.at[pl.ds(0, 4), :, pl.ds(0, 2 * FB)]
    og[...] = own_grads(range(4))
    arrived(1)
    start(3, 7)
    og[...] += own_grads(range(4, NT))
    ogc = pltpu.make_async_copy(og, og_hbm, sw.at[2])
    ogc.start()
    for i in range(NT // 2):
        for cp in outs(2 * i, 0, True):
            cp.wait()
    arrived(3)
    start(17, 18)

    def relay(k):
        qb[k] = (rb[2 * k:2 * k + 2, :, blk(*far[k])].astype(f32) + r0[k].astype(f32)).astype(bf16)

    def group_sum(k):
        fin[k] = (rb[2 * k:2 * k + 2, :, blk(yi, xi)].astype(f32) + r1[k].astype(f32)
                  + r2[k].astype(f32)).astype(bf16)

    def total(k):
        zf[2 * k:2 * k + 2] = fin[k].astype(f32) + rz[k].astype(f32)

    def at5():
        arrived(14)
        relay(0)
        start(20)
        arrived(4)
        start(6)

    def at6():
        arrived(15)
        relay(1)
        start(21)

    def at7():
        arrived(7, 8)
        start(9, 10)
        arrived(16)
        relay(2)
        start(22, 19)

    def at8():
        arrived(5, 6)

    def at10():
        arrived(17, 20)
        group_sum(0)
        start(23)

    def at11():
        arrived(18, 21)
        group_sum(1)
        start(24)
        arrived(9)
        start(11)

    def at12():
        arrived(10, 11)
        arrived(19, 22)
        group_sum(2)
        start(25)

    def zown(q):
        sl = zp[q]
        return pltpu.make_async_copy(zf.at[sl], z_hbm.at[pl.ds(ci * 6 + sl.start, sl.size)], sg.at[q])

    def at15():
        arrived(23, 24)
        total(0)
        total(1)
        start(26)
        zown(0).start()

    events = {5: at5, 6: at6, 7: at7, 8: at8, 10: at10, 11: at11}

    def phase1(i, c):
        for k, ev in events.items():
            pl.when(i == k)(ev)
        tiles(i, False)
        return c

    def phase2(i, c):
        pl.when(i == 15)(at15)
        tiles(i, False, last=True)
        return c

    n = NF * NT
    lax.fori_loop(NT // 2, 12, phase1, 0)
    at12()
    lax.fori_loop(12, n // 2, phase2, 0)
    ocp(n - 5, 0, 1).wait()
    dxp(n - 1, 1, 1, False, 0)
    ocp(n - 1, 0, 1).start()
    zoth = [pltpu.make_async_copy(zr.at[sl], z_hbm.at[pl.ds(6 - ci * 6 + sl.start, sl.size)], sw.at[q])
            for q, sl in enumerate(zp)]
    arrived(25)
    total(2)
    start(27)
    zown(1).start()
    arrived(26)
    zoth[0].start()
    for q in (0, 1):
        for cp in outs(n - 4 + 2 * q, q):
            cp.wait()
        ocp(n - 4 + 2 * q, q, 0).wait()
    ocp(n - 3, 1, 1).wait()
    for k in range(len(table)):
        rc(k).wait_send()
    arrived(27)
    zoth[1].start()
    ocp(n - 1, 0, 1).wait()
    for cp in zoth + [zown(0), zown(1), ogc]:
        cp.wait()


def call_a(x, dy, w1, w3, w2, g):
    part = (3, 2, 144, FB)
    dma = pltpu.SemaphoreType.DMA
    return pl.pallas_call(
        kernel_a,
        out_shape=(jax.ShapeDtypeStruct((D, T), bf16), jax.ShapeDtypeStruct((3, F, T), bf16),
                   jax.ShapeDtypeStruct((12, 144, FB), f32),
                   jax.ShapeDtypeStruct((4, 144, 2 * FB), f32)),
        in_specs=[ANY] * 6, out_specs=[ANY] * 4,
        scratch_shapes=[
            pltpu.VMEM((NT, D, TB), bf16), pltpu.VMEM((NT, D, TB), bf16),
            pltpu.VMEM((2, 3, FB, TB), f32), *[pltpu.VMEM((4, 3, FB, TB), bf16)] * 2,
            pltpu.VMEM((NT, D, TB), f32),
            *[pltpu.VMEM((2, D, TB), bf16)] * 2,
            pltpu.VMEM((NF, 3, FB, D), bf16),
            pltpu.VMEM((6, 144, F), f32), *[pltpu.VMEM((6, 144, F), bf16)] * 2,
            *[pltpu.VMEM(part, bf16)] * 6, *[pltpu.VMEM((6, 144, FB), f32)] * 2,
            dma((NT,)), dma((NT,)), dma((4, 2)), dma((2, 2)), dma((3,)), dma((2,)),
            dma((28,)), dma((28,))],
        compiler_params=pltpu.CompilerParams(vmem_limit_bytes=67043328, collective_id=0,
                                             has_side_effects=True),
        name="fwd_dx")(x, dy, w1, w3, w2, g)


def kernel_b(x_hbm, dy_hbm, r_hbm, dxi_hbm, z_hbm, og_hbm, o_hbm, dx_hbm, n_hbm,
             xy, r0, r, o0, o, dxb, ogb, zb, zt, sx, s0, so0, sdy, sr, so, sdx, sog, sz, sn):
    yi, fi = lax.axis_index("fo"), lax.axis_index("fi")
    xi, ci = fi // 2, fi % 2

    def cols(b, n):
        return pl.ds(pl.multiple_of(b * n, n), n)

    def tri(src, dst, sem):
        return pltpu.make_async_copy(src, dst, sem)

    nb = cols(yi * 2 + 1 - xi, FB)
    mine = cols(yi * 2 + xi, FB)
    ks = [pl.ds(k * KC, KC) for k in range(T // KC)]
    first = [[tri(x_hbm.at[:, k], xy.at[0, :, k], sx.at[q])]
             + [tri(r_hbm.at[m, nb, k], r0.at[pl.ds(m * FB, FB), k], s0.at[m, q]) for m in (0, 1)]
             for q, k in enumerate(ks)]
    o0c = [tri(o0.at[:, pl.ds(m * FB, FB)], o_hbm.at[m, :, nb], so0.at[m]) for m in (0, 1)]
    dyc = tri(dy_hbm, xy.at[1], sdy)
    dxin, dxout = tri(dxi_hbm, dxb, sdx.at[0]), tri(dxb, dx_hbm, sdx.at[1])
    ogin = tri(og_hbm, ogb, sog.at[2])
    ogout = [tri(ogb.at[:, pl.ds(m * FB, FB)], o_hbm.at[m, :, mine], sog.at[m]) for m in (0, 1)]

    def place(s):
        return s - s // 3, cols((1 - s // 2) * (1 - yi) + s // 3, BN)

    def rcp(s):
        m, c = place(s)
        return tri(r_hbm.at[m, c, :], r.at[s % 2], sr.at[s % 2])

    def ocp(s):
        m, c = place(s)
        return tri(o.at[s % 2], o_hbm.at[m, :, c], so.at[s % 2])

    def zcp(m):
        return tri(z_hbm.at[m], zb.at[m], sz.at[m])

    def ncp(m):
        return tri(zt.at[m, cols(ci, FB // 2), :], n_hbm.at[m], sn.at[m])

    for cps in first:
        for cp in cps:
            cp.start()
    rcp(0).start()
    rcp(1).start()
    for m in range(3):
        zcp(m).start()
    dyc.start()
    zb[3] = jnp.zeros(zb.shape[1:], f32)
    for q, cps in enumerate(first):
        for cp in cps:
            cp.wait()
        v = lax.dot_general(xy[0, :, ks[q]], r0[:, ks[q]], NTD, preferred_element_type=f32)
        o0[...] = v if q == 0 else o0[...] + v
    for cp in o0c:
        cp.start()

    def step(s, c):
        pl.when(s == 2)(dyc.wait)

        @pl.when(s == 3)
        def _():
            dxin.wait()
            dxout.start()
            ogin.wait()
            for cp in ogout:
                cp.start()

        @pl.when(s > 0)
        def _():
            zcp(s - 1).wait()

        rcp(s).wait()
        pl.when(s > 1)(ocp(s - 2).wait)
        o[s % 2] = lax.dot_general(xy[s // 2], r[s % 2], NTD, preferred_element_type=f32)
        zt[(s + 3) % 4] = zb[(s + 3) % 4].T
        ocp(s).start()

        @pl.when(s > 0)
        def _():
            ncp(s - 1).start()

        @pl.when(s < 2)
        def _():
            rcp(s + 2).start()

        pl.when(s == 0)(dxin.start)
        pl.when(s == 1)(ogin.start)
        return c

    lax.fori_loop(0, 4, step, 0)
    for cp in o0c + ogout + [dxout, ocp(2), ocp(3)] + [ncp(m) for m in range(3)]:
        cp.wait()


BN, KC = 2 * FB, 1024


def call_b(x, dy, r, dxi, z, og):
    dma = pltpu.SemaphoreType.DMA
    return pl.pallas_call(
        kernel_b,
        out_shape=(jax.ShapeDtypeStruct((3, D, F), f32), jax.ShapeDtypeStruct((D, T), bf16),
                   jax.ShapeDtypeStruct((3, FB // 2, D), f32)),
        in_specs=[ANY] * 6, out_specs=[ANY] * 3,
        scratch_shapes=[
            pltpu.VMEM((2, D, T), bf16), pltpu.VMEM((BN, T), bf16), pltpu.VMEM((2, BN, T), bf16),
            pltpu.VMEM((D, BN), f32), pltpu.VMEM((2, D, BN), f32), pltpu.VMEM((D, T), bf16),
            pltpu.VMEM((D, BN), f32), pltpu.VMEM((4, D, FB), f32), pltpu.VMEM((4, FB, D), f32),
            dma((4,)), dma((2, 4)), dma((2,)), dma, dma((2,)), dma((2,)), dma((2,)), dma((3,)),
            dma((3,)), dma((3,))],
        compiler_params=pltpu.CompilerParams(vmem_limit_bytes=60 << 20),
        name="wgrad")(x, dy, r, dxi, z, og)


def solution(mesh):
    grp = ("fo", "fi")
    alla = ("dp", "fo", "fi")

    def local(x, dy, w1s, w3s, w2s, g):
        dx, r, z, og = call_a(x.T, dy.T, w1s.T, w3s.T, w2s, g.reshape(12, 144, F))
        dwl, dx, dwn = call_b(x.T, dy.T, r, dx, z.reshape(3, D, FB), og.reshape(D, BN))
        return dx.T, dwn.transpose(0, 2, 1), dwl[None]

    return jax.shard_map(
        local, mesh=mesh,
        in_specs=(P(alla, None), P(alla, None), P(None, grp), P(None, grp), P(grp, None),
                  P(alla, None, None, None)),
        out_specs=(P(alla, None), P(None, None, grp), P(alla, None, None, None)),
        check_vma=False)
```

```python
import jax
import jax.numpy as jnp
from jax import lax
from jax.experimental import pallas as pl
from jax.experimental.pallas import tpu as pltpu
from jax.sharding import PartitionSpec as P

bf16, f32 = jnp.bfloat16, jnp.float32
T, D, F = 4096, 576, 1536
FB, TB, RC = 384, 512, 16
NF, NT = F // FB, T // TB
NN = (((1,), (0,)), ((), ()))
NTD = (((1,), (1,)), ((), ()))
ANY = pl.BlockSpec(memory_space=pl.ANY)
VM = pl.BlockSpec(memory_space=pltpu.VMEM)


def dot(a, b):
    return lax.dot_general(a, b, NN, preferred_element_type=f32)


def kernel_a(x_hbm, dy_hbm, w1_hbm, w3_hbm, w2_hbm, g_hbm, dx_hbm, r_hbm, z_hbm, og_hbm,
             x, dy, acts, dda, ddb, dxa, dxoa, dxob, wg, gst, sb, rb, r0, r1, r2,
             qb, fin, rz, zf, zr,
             sx, sd, so, sdx, sw, sg, ssem, rsem):
    dd, dxo = (dda, ddb), (dxoa, dxob)
    zi, yi, fi = lax.axis_index("dp"), lax.axis_index("fo"), lax.axis_index("fi")
    xi, ci = fi // 2, fi % 2
    to_c = (zi, yi, xi * 2 + 1 - ci)
    to_x = (zi, yi, (1 - xi) * 2 + ci)
    to_y = (zi, 1 - yi, fi)
    to_z = (1 - zi, yi, fi)
    own = ci * 192
    half, other = own + zi * 96, own + (1 - zi) * 96

    def blk(yy, xx):
        return pl.ds(pl.multiple_of((yy * 2 + xx) * FB, FB), FB)

    def wrows(j, r, n):
        return wg.at[j, :, pl.ds(pl.multiple_of(r, 16), n), :]

    def piece(k, yy, xx):
        return rb.at[pl.ds(2 * k, 2), :, blk(yy, xx)]

    table = [
        (wrows(0, own, 192), wrows(0, own, 192), to_c),
        (wrows(0, own, 192), wrows(1, own, 192), to_x),
        (wrows(0, half, 96), wrows(2, half, 96), to_y),
        (wrows(1, own, 192), wrows(1, own, 192), to_c),
        (wrows(2, half, 96), wrows(2, half, 96), to_z),
        (wrows(2, half, 96), wrows(2, half, 96), to_c),
        (wrows(2, other, 96), wrows(2, other, 96), to_c),
        (wrows(1, half, 48), wrows(3, half, 48), to_y),
        (wrows(2, half + 48, 48), wrows(3, half + 48, 48), to_x),
        (wrows(3, half, 96), wrows(3, half, 96), to_z),
        (wrows(3, half, 96), wrows(3, half, 96), to_c),
        (wrows(3, other, 96), wrows(3, other, 96), to_c),
    ]
    yo, xo = 1 - yi, 1 - xi
    fst, snd = (to_y, to_y, to_x), (to_x, to_x, to_y)
    far, near = ((yi, xo), (yi, xo), (yo, xi)), ((yo, xi), (yo, xi), (yi, xo))
    zp = (pl.ds(0, 4), pl.ds(4, 2))
    table += [(sb.at[pl.ds(k, 3)], rb.at[pl.ds(k, 3)], to_c) for k in (0, 3)]
    table += [(piece(k, yo, xo), r0.at[k], fst[k]) for k in range(3)]
    table += [(piece(k, *near[k]), r1.at[k], fst[k]) for k in range(3)]
    table += [(qb.at[k], r2.at[k], snd[k]) for k in range(3)]
    table += [(fin.at[k], rz.at[k], to_z) for k in range(3)]
    table += [(zf.at[sl], zr.at[sl], to_c) for sl in zp]

    def rc(k):
        src, dst, dev = table[k]
        return pltpu.make_async_remote_copy(src, dst, ssem.at[k], rsem.at[k], device_id=dev,
                                            device_id_type=pl.DeviceIdType.MESH)

    def start(*ks):
        for k in ks:
            rc(k).start()

    def arrived(*ks):
        for k in ks:
            rc(k).wait_recv()

    def xcp(t):
        return pltpu.make_async_copy(x_hbm.at[:, pl.ds(t * TB, TB)], x.at[t], sx.at[t])

    def dcp(t):
        return pltpu.make_async_copy(dy_hbm.at[:, pl.ds(t * TB, TB)], dy.at[t], sd.at[t])

    def gcp(i, side):
        return pltpu.make_async_copy(g_hbm.at[pl.ds(side * 6 + i * 3, 3)], gst.at[pl.ds(i * 3, 3)], sg.at[i])

    wcps = [pltpu.make_async_copy(h, wg.at[0, m, pl.ds(pl.multiple_of(own, 192), 192), :], sw.at[m])
            for m, h in enumerate((w1_hbm, w3_hbm, w2_hbm))]
    bar = pltpu.get_barrier_semaphore()
    for dev in (to_c, to_x, to_y, to_z):
        pl.semaphore_signal(bar, inc=1, device_id=dev, device_id_type=pl.DeviceIdType.MESH)
    for cp in wcps:
        cp.start()
    xcp(0).start()
    dcp(0).start()
    xcp(1).start()
    dcp(1).start()
    for i in (0, 1):
        gcp(i, 1 - ci).start()
    for t in range(2, NT):
        xcp(t).start()
        dcp(t).start()
    ddb[3] = jnp.zeros(ddb.shape[1:], bf16)
    for cp in wcps:
        cp.wait()
    pl.semaphore_wait(bar, 4)
    start(1, 2, 0)

    def outs(s0, q, first=False):
        j = s0 // NT
        yj = yi + (j // 2) * (1 - 2 * yi)
        xj = xi + (j % 2) * (1 - 2 * xi)
        fs = blk(yj, xj)
        w, m = (s0 // 2, 2) if first else (q, slice(None))
        return [pltpu.make_async_copy(
            dd[p].at[w, m], r_hbm.at[m, fs, pl.ds(pl.multiple_of((s0 + p) % NT * TB, TB), TB)],
            so.at[w, p]) for p in (0, 1)]

    def fwd(f, t, p):
        acts[p, 0] = dot(wg[f, 0], x[t])
        acts[p, 1] = dot(wg[f, 1], x[t])
        acts[p, 2] = dot(wg[f, 2], dy[t])

    def ew(p, w):
        for r in range(0, FB, RC):
            a, b, dh = (acts[p, k, r:r + RC, :] for k in range(3))
            s = 0.5 * jnp.tanh(0.5 * a) + 0.5
            sa = a * s
            dd[p][w, 2, r:r + RC, :] = (sa * b).astype(bf16)
            dd[p][w, 0, r:r + RC, :] = (dh * b * (s * (1.0 + a * (1.0 - s)))).astype(bf16)
            dd[p][w, 1, r:r + RC, :] = (dh * sa).astype(bf16)

    def ocp(s, q, p):
        ts = pl.ds(pl.multiple_of(s % NT * TB, TB), TB)
        return pltpu.make_async_copy(dxo[p].at[q], dx_hbm.at[:, ts], sdx.at[q, p])

    def tdot(j, b):
        return lax.dot_general(wg[j, :2].reshape(2 * FB, D), b, (((0,), (0,)), ((), ())),
                               preferred_element_type=f32)

    def dab(p, w):
        return dd[p][w, :2].reshape(2 * FB, TB)

    def dxp(s, q, p, first, o=None):
        t = s % NT
        if first:
            dxa[t] = tdot(0, dab(p, q))
            return
        v = dxa[t] + tdot(s // NT, dab(p, q))
        dxa[t] = v
        if o is not None:
            dxo[p][o] = v.astype(bf16)

    def tiles(i, first, extra=None, last=False):
        s0, q = 2 * i, i % 2
        w = i if first else q
        prev = (i + 3) % 4 if first else 1 - q if last else 1 - q + 2 * ((11 - i) // 7)
        f, t0 = s0 // NT, s0 % NT

        if not first:
            @pl.when(i > 5)
            def _():
                for cp in outs(s0 - 4, q):
                    cp.wait()

        if last:
            @pl.when(i > 13)
            def _():
                ocp(s0 - 5, q, 1).wait()
                ocp(s0 - 4, q, 0).wait()

        o = q if last else None
        fwd(f, t0, 0)
        ew(0, w)
        if extra is not None:
            extra(0)
        dxp(s0 + NT - 1 if first else s0 - 1, prev, 1, first, o)
        fwd(f, t0 + 1, 1)
        ew(1, w)
        if extra is not None:
            extra(1)
        dxp(s0, w, 0, first, o)
        for cp in outs(s0, q, first):
            cp.start()
        if last:
            ocp(s0 - 1, q, 1).start()
            ocp(s0, q, 0).start()

    def need(i):
        for t in (2 * i, 2 * i + 1):
            xcp(t).wait()
            dcp(t).wait()

    def phase0a(i, c):
        need(i)
        gcp(i, 1 - ci).wait()

        def conv(h):
            for gr in range(3):
                for r in range(72 * h, 72 * h + 72, 24):
                    sb[i * 3 + gr, r:r + 24, :] = gst[i * 3 + gr, r:r + 24, :].astype(bf16)

        tiles(i, True, conv)

        @pl.when(i == 0)
        def _():
            start(12)

        @pl.when(i == 1)
        def _():
            start(13)

        gcp(i, ci).start()
        return c

    def phase0b(i, c):
        need(i + 2)
        gcp(i, ci).wait()

        @pl.when(i == 0)
        def _():
            arrived(12)

        @pl.when(i == 1)
        def _():
            arrived(13)
            start(14)
            arrived(2)
            start(4, 5, 8)

        def conv(h):
            for gr in range(3):
                for r in range(72 * h, 72 * h + 72, 24):
                    v = gst[i * 3 + gr, r:r + 24, :].astype(bf16).astype(f32)
                    v = v + rb[i * 3 + gr, r:r + 24, :].astype(f32)
                    rb[i * 3 + gr, r:r + 24, :] = v.astype(bf16)

        tiles(i + 2, True, conv)
        return c

    arrived(0)
    lax.fori_loop(0, 2, phase0a, 0)
    lax.fori_loop(0, 2, phase0b, 0)
    start(15, 16)
    def own_grads(ts):
        return sum(lax.dot_general(x[t], dab(t % 2, t // 2), NTD, preferred_element_type=f32)
                   for t in ts).reshape(4, 144, 2 * FB)

    og = gst.at[pl.ds(0, 4), :, pl.ds(0, 2 * FB)]
    og[...] = own_grads(range(4))
    arrived(1)
    start(3, 7)
    og[...] += own_grads(range(4, NT))
    ogc = pltpu.make_async_copy(og, og_hbm, sw.at[2])
    ogc.start()
    for i in range(NT // 2):
        for cp in outs(2 * i, 0, True):
            cp.wait()
    arrived(3)
    start(17, 18)

    def relay(k):
        qb[k] = (rb[2 * k:2 * k + 2, :, blk(*far[k])].astype(f32) + r0[k].astype(f32)).astype(bf16)

    def group_sum(k):
        fin[k] = (rb[2 * k:2 * k + 2, :, blk(yi, xi)].astype(f32) + r1[k].astype(f32)
                  + r2[k].astype(f32)).astype(bf16)

    def total(k):
        zf[2 * k:2 * k + 2] = fin[k].astype(f32) + rz[k].astype(f32)

    def at5():
        arrived(14)
        relay(0)
        start(20)
        arrived(4)
        start(6)

    def at6():
        arrived(15)
        relay(1)
        start(21)

    def at7():
        arrived(7, 8)
        start(9, 10)
        arrived(16)
        relay(2)
        start(22, 19)

    def at8():
        arrived(5, 6)

    def at10():
        arrived(17, 20)
        group_sum(0)
        start(23)

    def at11():
        arrived(18, 21)
        group_sum(1)
        start(24)
        arrived(9)
        start(11)

    def at12():
        arrived(10, 11)
        arrived(19, 22)
        group_sum(2)
        start(25)

    def zown(q):
        sl = zp[q]
        return pltpu.make_async_copy(zf.at[sl], z_hbm.at[pl.ds(ci * 6 + sl.start, sl.size)], sg.at[q])

    def at15():
        arrived(23, 24)
        total(0)
        total(1)
        start(26)
        zown(0).start()

    events = {5: at5, 6: at6, 7: at7, 8: at8, 10: at10, 11: at11}

    def phase1(i, c):
        for k, ev in events.items():
            pl.when(i == k)(ev)
        tiles(i, False)
        return c

    def phase2(i, c):
        pl.when(i == 15)(at15)
        tiles(i, False, last=True)
        return c

    n = NF * NT
    lax.fori_loop(NT // 2, 12, phase1, 0)
    at12()
    lax.fori_loop(12, n // 2, phase2, 0)
    ocp(n - 5, 0, 1).wait()
    dxp(n - 1, 1, 1, False, 0)
    ocp(n - 1, 0, 1).start()
    zoth = [pltpu.make_async_copy(zr.at[sl], z_hbm.at[pl.ds(6 - ci * 6 + sl.start, sl.size)], sw.at[q])
            for q, sl in enumerate(zp)]
    arrived(25)
    total(2)
    start(27)
    zown(1).start()
    arrived(26)
    zoth[0].start()
    for q in (0, 1):
        for cp in outs(n - 4 + 2 * q, q):
            cp.wait()
        ocp(n - 4 + 2 * q, q, 0).wait()
    ocp(n - 3, 1, 1).wait()
    for k in range(len(table)):
        rc(k).wait_send()
    arrived(27)
    zoth[1].start()
    ocp(n - 1, 0, 1).wait()
    for cp in zoth + [zown(0), zown(1), ogc]:
        cp.wait()


def call_a(x, dy, w1, w3, w2, g):
    part = (3, 2, 144, FB)
    dma = pltpu.SemaphoreType.DMA
    return pl.pallas_call(
        kernel_a,
        out_shape=(jax.ShapeDtypeStruct((D, T), bf16), jax.ShapeDtypeStruct((3, F, T), bf16),
                   jax.ShapeDtypeStruct((12, 144, FB), f32),
                   jax.ShapeDtypeStruct((4, 144, 2 * FB), f32)),
        in_specs=[ANY] * 6, out_specs=[ANY] * 4,
        scratch_shapes=[
            pltpu.VMEM((NT, D, TB), bf16), pltpu.VMEM((NT, D, TB), bf16),
            pltpu.VMEM((2, 3, FB, TB), f32), *[pltpu.VMEM((4, 3, FB, TB), bf16)] * 2,
            pltpu.VMEM((NT, D, TB), f32),
            *[pltpu.VMEM((2, D, TB), bf16)] * 2,
            pltpu.VMEM((NF, 3, FB, D), bf16),
            pltpu.VMEM((6, 144, F), f32), *[pltpu.VMEM((6, 144, F), bf16)] * 2,
            *[pltpu.VMEM(part, bf16)] * 6, *[pltpu.VMEM((6, 144, FB), f32)] * 2,
            dma((NT,)), dma((NT,)), dma((4, 2)), dma((2, 2)), dma((3,)), dma((2,)),
            dma((28,)), dma((28,))],
        compiler_params=pltpu.CompilerParams(vmem_limit_bytes=67043328, collective_id=0,
                                             has_side_effects=True),
        name="fwd_dx")(x, dy, w1, w3, w2, g)


def kernel_b(x_hbm, dy_hbm, r_hbm, dxi_hbm, z_hbm, og_hbm, o_hbm, dx_hbm, n_hbm,
             xy, r0, r, o0, o, dxb, ogb, zb, zt, sx, s0, so0, sdy, sr, so, sdx, sog, sz, sn):
    yi, fi = lax.axis_index("fo"), lax.axis_index("fi")
    xi, ci = fi // 2, fi % 2

    def cols(b, n):
        return pl.ds(pl.multiple_of(b * n, n), n)

    def tri(src, dst, sem):
        return pltpu.make_async_copy(src, dst, sem)

    nb = cols(yi * 2 + 1 - xi, FB)
    mine = cols(yi * 2 + xi, FB)
    ks = [pl.ds(k * KC, KC) for k in range(T // KC)]
    first = [[tri(x_hbm.at[:, k], xy.at[0, :, k], sx.at[q])]
             + [tri(r_hbm.at[m, nb, k], r0.at[pl.ds(m * FB, FB), k], s0.at[m, q]) for m in (0, 1)]
             for q, k in enumerate(ks)]
    o0c = [tri(o0.at[:, pl.ds(m * FB, FB)], o_hbm.at[m, :, nb], so0.at[m]) for m in (0, 1)]
    dyc = tri(dy_hbm, xy.at[1], sdy)
    dxin, dxout = tri(dxi_hbm, dxb, sdx.at[0]), tri(dxb, dx_hbm, sdx.at[1])
    ogin = tri(og_hbm, ogb, sog.at[2])
    ogout = [tri(ogb.at[:, pl.ds(m * FB, FB)], o_hbm.at[m, :, mine], sog.at[m]) for m in (0, 1)]

    def place(s):
        return s - s // 3, cols((1 - s // 2) * (1 - yi) + s // 3, BN)

    def rcp(s):
        m, c = place(s)
        return tri(r_hbm.at[m, c, :], r.at[s % 2], sr.at[s % 2])

    def ocp(s):
        m, c = place(s)
        return tri(o.at[s % 2], o_hbm.at[m, :, c], so.at[s % 2])

    def zcp(m):
        return tri(z_hbm.at[m], zb.at[m], sz.at[m])

    def ncp(m):
        return tri(zt.at[m, cols(ci, FB // 2), :], n_hbm.at[m], sn.at[m])

    for cps in first:
        for cp in cps:
            cp.start()
    rcp(0).start()
    rcp(1).start()
    for m in range(3):
        zcp(m).start()
    dyc.start()
    zb[3] = jnp.zeros(zb.shape[1:], f32)
    for q, cps in enumerate(first):
        for cp in cps:
            cp.wait()
        v = lax.dot_general(xy[0, :, ks[q]], r0[:, ks[q]], NTD, preferred_element_type=f32)
        o0[...] = v if q == 0 else o0[...] + v
    for cp in o0c:
        cp.start()

    def step(s, c):
        pl.when(s == 2)(dyc.wait)

        @pl.when(s == 3)
        def _():
            dxin.wait()
            dxout.start()
            ogin.wait()
            for cp in ogout:
                cp.start()

        @pl.when(s > 0)
        def _():
            zcp(s - 1).wait()

        rcp(s).wait()
        pl.when(s > 1)(ocp(s - 2).wait)
        o[s % 2] = lax.dot_general(xy[s // 2], r[s % 2], NTD, preferred_element_type=f32)
        zt[(s + 3) % 4] = zb[(s + 3) % 4].T
        ocp(s).start()

        @pl.when(s > 0)
        def _():
            ncp(s - 1).start()

        @pl.when(s < 2)
        def _():
            rcp(s + 2).start()

        pl.when(s == 0)(dxin.start)
        pl.when(s == 1)(ogin.start)
        return c

    lax.fori_loop(0, 4, step, 0)
    for cp in o0c + ogout + [dxout, ocp(2), ocp(3)] + [ncp(m) for m in range(3)]:
        cp.wait()


BN, KC = 2 * FB, 1024


def call_b(x, dy, r, dxi, z, og):
    dma = pltpu.SemaphoreType.DMA
    return pl.pallas_call(
        kernel_b,
        out_shape=(jax.ShapeDtypeStruct((3, D, F), f32), jax.ShapeDtypeStruct((D, T), bf16),
                   jax.ShapeDtypeStruct((3, FB // 2, D), f32)),
        in_specs=[ANY] * 6, out_specs=[ANY] * 3,
        scratch_shapes=[
            pltpu.VMEM((2, D, T), bf16), pltpu.VMEM((BN, T), bf16), pltpu.VMEM((2, BN, T), bf16),
            pltpu.VMEM((D, BN), f32), pltpu.VMEM((2, D, BN), f32), pltpu.VMEM((D, T), bf16),
            pltpu.VMEM((D, BN), f32), pltpu.VMEM((4, D, FB), f32), pltpu.VMEM((4, FB, D), f32),
            dma((4,)), dma((2, 4)), dma((2,)), dma, dma((2,)), dma((2,)), dma((2,)), dma((3,)),
            dma((3,)), dma((3,))],
        compiler_params=pltpu.CompilerParams(vmem_limit_bytes=60 << 20),
        name="wgrad")(x, dy, r, dxi, z, og)


def solution(mesh):
    grp = ("fo", "fi")
    alla = ("dp", "fo", "fi")

    def local(x, dy, w1s, w3s, w2s, g):
        dx, r, z, og = call_a(x.T, dy.T, w1s.T, w3s.T, w2s, g.reshape(12, 144, F))
        dwl, dx, dwn = call_b(x.T, dy.T, r, dx, z.reshape(3, D, FB), og.reshape(D, BN))
        return dx.T, dwn.transpose(0, 2, 1), dwl[None]

    return jax.shard_map(
        local, mesh=mesh,
        in_specs=(P(alla, None), P(alla, None), P(None, grp), P(None, grp), P(grp, None),
                  P(alla, None, None, None)),
        out_specs=(P(alla, None), P(None, None, grp), P(alla, None, None, None)),
        check_vma=False)
```
